32 devices in a mesh: seq: 16 (over z, y, x), head: 2 (over core).
Axes of the slice: x: 2, y: 2, z: 4, core: 2. Of those that a mesh axis runs over, the one named last changes fastest.
Arguments:
- hidden_state: bfloat16 [8, 4096], replicated, may hold values from -18 to 18
- query_weight: bfloat16 [4096, 2, 2048], P('seq', 'head'), may hold values from -1 to 1
- up_key: bfloat16 [2, 256, 512], P('head'), may hold values from -1 to 1
- up_value: bfloat16 [2, 256, 512], P('head'), may hold values from -0.375 to 0.375
- latent_key: bfloat16 [8, 16384, 2, 256], P(None, 'seq', 'head'), may hold values from -256 to 256
- latent_value: bfloat16 [8, 16384, 2, 256], P(None, 'seq', 'head'), may hold values from -6 to 6
- lengths: int32 [8], replicated, may hold values from 12288 to 16384
- block_mask: int32 [8, 64], P(None, 'seq'), may hold values from 0 to 1, as said below
- out_weight: bfloat16 [2, 2048, 4096], P('head', 'seq'), may hold values from -0.09375 to 0.09375
Outputs:
- attn_out: float32 [8, 4096], replicated
The draws below stay inside these ranges and needn't reach their ends.
Inputs may be any that keep to these rules, and one draw needn't show every extreme that they name: `block_mask`: blocks 0 and 32 of every sequence are valid.
All inputs are finite; a program needn't handle non-finite values.
Results may differ from the reference program's by a relative error of at most 0.0035.
Values sent between devices are 32-bit elements; how exact they have to be, the bound alone decides.
A program may use at most 64 MiB of HBM per device.

```python
import math
import jax
import jax.numpy as jnp
from jax import lax

D = 4096
HQ = 32
HD = 128
GROUPS = 2
R = 256
BLOCK = 256
B = 8
CTX_TOTAL = 16384
NBLK = 64
KPG = 4
REP = 4
QW = 2048
KW = 512


def common_parts(key):
    state = 3.0 * jax.random.truncated_normal(jax.random.fold_in(key, 11), -6.0, 6.0, (B, D), jnp.float32)
    weight = jax.random.truncated_normal(jax.random.fold_in(key, 12), -6.0, 6.0, (D, GROUPS, QW), jnp.float32) / math.sqrt(D)
    basis = jax.random.truncated_normal(jax.random.fold_in(key, 13), -6.0, 6.0, (GROUPS, R, KW), jnp.float32) / math.sqrt(R)
    return (state.astype(jnp.bfloat16), weight.astype(jnp.bfloat16), basis.astype(jnp.bfloat16))


def draw_hidden_state(key, part):
    return common_parts(key)[0]


def draw_query_weight(key, part):
    return common_parts(key)[1]


def draw_up_key(key, part):
    return common_parts(key)[2]


def draw_latent_key(key, part):
    base = jax.random.truncated_normal(jax.random.fold_in(key, 14), -6.0, 6.0, (B, CTX_TOTAL, GROUPS, R), jnp.float32)
    return base.astype(jnp.bfloat16)


def draw_block_mask(key, part):
    picks = jax.random.randint(jax.random.fold_in(key, 17), (B, NBLK), 0, 4)
    marks = jnp.where(picks > 0, 1, 0).astype(jnp.int32)
    return marks.at[:, 0].set(1).at[:, NBLK // 2].set(1)


def place_ends(array, rng, smallest, high):
    shape = array.shape
    index_at = [jax.random.randint(jax.random.fold_in(rng, axis), (), 0, shape[axis]) for axis in range(len(shape))]
    array = array.at[tuple(index_at)].set(smallest)
    longest = shape.index(max(shape))
    index_at[longest] = (index_at[longest] + 1) % shape[longest]
    return array.at[tuple(index_at)].set(high)


def level_of(stream_key, dims, split, least, top_value):
    loudness, own = 1.0, jax.random.fold_in(stream_key, 6)
    for position, parts in split:
        draws = jnp.exp(jax.random.uniform(jax.random.fold_in(own, position), (parts,), jnp.float32, least / len(split), top_value / len(split)))
        loudness = loudness * jnp.repeat(draws, dims[position] // parts).reshape([-1 if axis == position else 1 for axis in range(len(dims))])
    return loudness


def scatter_about(rng, dims, spread, limit, pieces=(), held_as=jnp.bfloat16):
    drawn = jax.random.normal(rng, dims, jnp.float32) * spread
    if len(pieces) > 0:
        drawn = level_of(rng, dims, pieces, -0.22, 0.18) * drawn
    return jnp.clip(drawn, min=-limit, max=limit).astype(held_as)


def setup_inputs(seed: int = 0) -> dict:
    streams_of = jax.random.split(jax.random.key(seed), 10)
    return {
        "hidden_state": draw_hidden_state(jax.random.fold_in(streams_of[9], 71), 0),
        "query_weight": draw_query_weight(jax.random.fold_in(streams_of[9], 71), 0),
        "up_key": draw_up_key(jax.random.fold_in(streams_of[9], 71), 0),
        "up_value": scatter_about(streams_of[3], (GROUPS, R, KW), R ** -0.5, 0.375, ((0, 2),)),
        "latent_key": draw_latent_key(jax.random.fold_in(streams_of[9], 71), 0),
        "latent_value": scatter_about(streams_of[5], (B, CTX_TOTAL, GROUPS, R), 1.0, 6.0, ((1, 16), (2, 2))),
        "lengths": place_ends(jax.random.randint(streams_of[6], (B,), CTX_TOTAL - CTX_TOTAL // 4, CTX_TOTAL + 1), jax.random.fold_in(streams_of[6], 1), CTX_TOTAL - CTX_TOTAL // 4, CTX_TOTAL).astype(jnp.int32),
        "block_mask": draw_block_mask(jax.random.fold_in(streams_of[9], 71), 0),
        "out_weight": scatter_about(streams_of[8], (GROUPS, QW, D), (HQ * HD) ** -0.5, 0.09375, ((0, 2), (1, 16))),
    }


def reference(hidden_state, query_weight, up_key, up_value, latent_key, latent_value, lengths, block_mask, out_weight):
    highest = lax.Precision.HIGHEST
    query = jnp.dot(hidden_state.astype(jnp.float32), query_weight.reshape(D, GROUPS * QW).astype(jnp.float32), preferred_element_type=jnp.float32)
    query_heads = query.reshape(B, GROUPS, KPG, REP, HD)
    positions = jnp.arange(CTX_TOTAL, dtype=jnp.int32)
    block_full = jnp.repeat(block_mask, BLOCK, axis=1)
    valid = (positions[None, :] < lengths[:, None]) & (block_full > 0)
    key_maps = up_key.astype(jnp.float32).reshape(GROUPS, R, KPG, HD)
    value_maps = up_value.astype(jnp.float32).reshape(GROUPS, R, KPG, HD)
    scale = 1.0 / math.sqrt(HD)

    def one_sequence(items):
        query_one, keys_one, values_one, valid_one = items
        results = []
        for group in range(GROUPS):
            query_latent = jnp.einsum('jrd,ejd->jre', query_one[group], key_maps[group], precision=highest)
            scores = jnp.einsum('jre,ce->jrc', query_latent, keys_one[:, group].astype(jnp.float32), precision=highest) * scale
            mask_one = valid_one[None, None, :]
            top = lax.optimization_barrier(jnp.max(jnp.where(mask_one, scores, -1e+30), axis=-1))
            weights = jnp.where(mask_one, jnp.exp(scores - top[..., None]), 0.0)
            total = lax.optimization_barrier(jnp.sum(weights, axis=-1))
            latent_sum = jnp.einsum('jrc,ce->jre', weights, values_one[:, group].astype(jnp.float32), precision=highest)
            summed = jnp.einsum('jre,ejd->jrd', latent_sum, value_maps[group], precision=highest)
            results.append(summed / total[..., None])
        return jnp.stack(results)
    context = lax.map(one_sequence, (query_heads, latent_key, latent_value, valid))
    context = context.reshape(B, GROUPS * QW).astype(jnp.bfloat16)
    result = jnp.dot(context.astype(jnp.float32), out_weight.reshape(GROUPS * QW, D).astype(jnp.float32), preferred_element_type=jnp.float32)
    return result
```

```python
import functools
import math

import jax
import jax.numpy as jnp
from jax import lax
from jax.experimental import pallas as pl
from jax.experimental.pallas import tpu as pltpu
from jax.sharding import PartitionSpec as P

HD = 128
BLOCK = 256
KPG = 4
REP = 4
MESH = pl.DeviceIdType.MESH
NEG = -1e30


def repeat(count, step):
    if count <= 32:
        for i in range(count):
            step(i)
    else:
        lax.fori_loop(0, count, lambda i, c: (step(i), c)[1], 0)


def halves(x):
    high = x.astype(jnp.bfloat16)
    low = (x - high.astype(jnp.float32)).astype(jnp.bfloat16)
    return jnp.concatenate([high, low], axis=0)


def dot_nt(a, b):
    return lax.dot_general(a, b, (((1,), (1,)), ((), ())), preferred_element_type=jnp.float32)


def strided(ref, first, count, stride):
    parts = [ref[k, pl.ds(first, count, stride=stride), :] for k in range(ref.shape[0])]
    return jnp.concatenate(parts, axis=1)


def folded(x):
    rows = x.shape[0] // 2
    return x[:rows] + x[rows:]


def kernel(
    n,
    cores,
    lengths,
    block_mask,
    hidden,
    query_weight,
    up_key,
    up_value,
    keys,
    values,
    out_weight,
    out,
    qw,
    uk,
    uv,
    kv,
    vv,
    ow,
    send1,
    recv1,
    send2,
    recv2,
    ql,
    ls,
    st,
    send3,
    recv3,
    send4,
    recv4,
    send5,
    recv5,
    load_sem,
    key_sem,
    value_sem,
    send_sem,
    recv_sem,
):
    me = lax.axis_index("seq")
    core = lax.axis_index("head")
    batch, context_len = keys.shape[0], keys.shape[1]
    heads = KPG * REP
    spread = n // heads
    my_head = me // spread
    chunks = out.shape[1] // HD
    per_head = chunks // heads
    my_chunk = my_head * per_head + core
    dim_rows, out_rows = query_weight.shape[0], out_weight.shape[0]
    owner = lax.rem(me, spread) == 0

    def local(src, dst, sem):
        return pltpu.make_async_copy(src, dst, sem)

    def remote(src, dst, phase, seq, head):
        return pltpu.make_async_remote_copy(
            src_ref=src,
            dst_ref=dst,
            send_sem=send_sem.at[phase],
            recv_sem=recv_sem.at[phase],
            device_id=(seq, head),
            device_id_type=MESH,
        )

    def to_either(here, src, dst, phase, seq, head):
        if here is True:
            local(src, dst, recv_sem.at[phase]).start()
        elif here is False:
            remote(src, dst, phase, seq, head).start()
        else:

            @pl.when(here)
            def _():
                local(src, dst, recv_sem.at[phase]).start()

            @pl.when(jnp.logical_not(here))
            def _():
                remote(src, dst, phase, seq, head).start()

    def wait_bytes(ref, sem):
        local(ref, ref, sem).wait()

    def when_owner(action):
        if spread == 1:
            action()
        else:
            pl.when(owner)(action)

    def first_is_here():
        return True if spread == 1 else owner

    if dim_rows >= HD:
        qw_at = qw
    else:
        qw_at = qw.at[pl.ds(pl.multiple_of(lax.rem(me * dim_rows, HD), dim_rows), dim_rows)]
    qw_copy = local(query_weight, qw_at, load_sem.at[0])
    qw_copy.start()

    barrier = pltpu.get_barrier_semaphore()
    devices = n * cores

    def greet(i):
        other = lax.rem(me * cores + core + i + 1, devices)
        pl.semaphore_signal(
            barrier, inc=1, device_id=(other // cores, lax.rem(other, cores)), device_id_type=MESH
        )

    repeat(devices - 1, greet)

    qw_copy.wait()
    uk_copy = local(up_key, uk, load_sem.at[1])
    uk_copy.start()
    key_copies = [local(keys.at[b], kv.at[b], key_sem.at[b]) for b in range(batch)]
    value_copies = [local(values.at[b], vv.at[b], value_sem.at[b]) for b in range(batch)]
    for b in range(batch):
        key_copies[b].start()
        value_copies[b].start()
    uv_copy = local(up_value, uv, load_sem.at[2])
    uv_copy.start()
    if out_rows >= HD:
        ow_at = ow
    else:
        ow_at = ow.at[pl.ds(pl.multiple_of(lax.rem(me * out_rows, HD), out_rows), out_rows)]
    ow_copy = local(out_weight, ow_at, load_sem.at[3])
    ow_copy.start()

    if dim_rows >= HD:
        state = hidden[:, pl.ds(pl.multiple_of(me * dim_rows, HD), dim_rows)]
        weight = qw[...]
    else:
        start = lax.rem(me * dim_rows, HD)
        state = hidden[:, pl.ds(pl.multiple_of(me * dim_rows - start, HD), HD)]
        row = lax.broadcasted_iota(jnp.int32, qw.shape, 0)
        weight = jnp.where((row >= start) & (row < start + dim_rows), qw[...].astype(jnp.float32), 0.0)
        weight = weight.astype(jnp.bfloat16)
    part = jnp.dot(state, weight, preferred_element_type=jnp.float32)
    for h in range(heads):
        send1[h] = part[:, h * HD : (h + 1) * HD]

    pl.semaphore_wait(barrier, devices - 1)

    for i in range(heads):
        h = lax.rem(my_head + i, heads)
        here = first_is_here() if i == 0 else False
        to_either(here, send1.at[h], recv1.at[me], 0, h * spread, core)

    def gather_query():
        wait_bytes(recv1, recv_sem.at[0])
        send2[...] = jnp.sum(recv1[...], axis=0)
        local(send2, recv2.at[my_head], recv_sem.at[1]).start()

        def send(i):
            remote(send2, recv2.at[my_head], 1, lax.rem(me + i + 1, n), core).start()

        repeat(n - 1, send)

    when_owner(gather_query)
    uk_copy.wait()
    wait_bytes(recv2, recv_sem.at[1])

    scale = 1.0 / math.sqrt(HD)
    rank = uk.shape[0]
    for j in range(KPG):
        rows = recv2[j * REP : (j + 1) * REP].reshape(REP * batch, HD)
        mapped = folded(dot_nt(halves(rows), uk[:, j * HD : (j + 1) * HD])) * scale
        for k in range(rank // HD):
            ql[k, j * REP * batch : (j + 1) * REP * batch, :] = mapped[:, k * HD : (k + 1) * HD]

    blocks = context_len // BLOCK
    lane = lax.broadcasted_iota(jnp.int32, (1, BLOCK), 1)
    stat_lane = lax.broadcasted_iota(jnp.int32, (heads, HD), 1)
    for b in range(batch):
        query = halves(strided(ql, b, heads, batch))
        key_copies[b].wait()
        scores = folded(dot_nt(query, kv[b]))
        limits = [
            jnp.where(block_mask[k, b] == 1, lengths[b] - me * context_len - k * BLOCK, 0)
            for k in range(blocks)
        ]
        valid = jnp.concatenate([lane < limit for limit in limits], axis=1)
        scores = jnp.where(valid, scores, NEG)
        peak = jnp.max(scores, axis=1, keepdims=True)
        weights = jnp.where(valid, jnp.exp(scores - peak), 0.0)
        total = jnp.sum(weights, axis=1, keepdims=True)
        value_copies[b].wait()
        latent = folded(jnp.dot(halves(weights), vv[b], preferred_element_type=jnp.float32))
        for k in range(rank // HD):
            ls[k, b * heads : (b + 1) * heads, :] = latent[:, k * HD : (k + 1) * HD]
        st[b * heads : (b + 1) * heads, :] = jnp.where(stat_lane < HD // 2, peak, total)

    uv_copy.wait()
    for j in range(KPG):
        rows = jnp.concatenate(
            [strided(ls, j * REP + r, batch, heads) for r in range(REP)], axis=0
        )
        summed = folded(
            jnp.dot(halves(rows), uv[:, j * HD : (j + 1) * HD], preferred_element_type=jnp.float32)
        )
        for r in range(REP):
            h = j * REP + r
            send3[h, 0:batch] = summed[r * batch : (r + 1) * batch]
            send3[h, batch : 2 * batch] = st[pl.ds(h, batch, stride=heads), :]

    local(send3.at[my_head], recv3.at[me], recv_sem.at[2]).start()

    def send_carry(i):
        target = lax.rem(me + i + 1, n)
        remote(send3.at[target // spread], recv3.at[me], 2, target, core).start()

    repeat(n - 1, send_carry)
    wait_bytes(recv3, recv_sem.at[2])

    stats = recv3[:, batch : 2 * batch, :]
    turned = pltpu.roll(stats, HD // 2, 2)
    low_lanes = lax.broadcasted_iota(jnp.int32, stats.shape, 2) < HD // 2
    peaks = jnp.where(low_lanes, stats, turned)
    totals = jnp.where(low_lanes, turned, stats)
    factor = jnp.exp(peaks - jnp.max(peaks, axis=0, keepdims=True))
    summed = jnp.sum(recv3[:, 0:batch, :] * factor, axis=0)
    context = (summed / jnp.sum(totals * factor, axis=0)).astype(jnp.bfloat16)

    ow_copy.wait()
    if out_rows >= HD:
        weight = ow[...]
    else:
        start = lax.rem(me * out_rows, HD)
        row = lax.broadcasted_iota(jnp.int32, ow.shape, 0)
        weight = jnp.where((row >= start) & (row < start + out_rows), ow[...].astype(jnp.float32), 0.0)
        weight = weight.astype(jnp.bfloat16)
    part = jnp.dot(context, weight, preferred_element_type=jnp.float32)
    for c in range(chunks):
        send4[c] = part[:, c * HD : (c + 1) * HD]

    for i in range(chunks):
        c = lax.rem(my_chunk + i, chunks)
        here = first_is_here() if i == 0 else False
        to_either(here, send4.at[c], recv4.at[me * cores + core], 3, c // per_head * spread, lax.rem(c, per_head))

    def gather_out():
        wait_bytes(recv4, recv_sem.at[3])
        send5[...] = jnp.sum(recv4[...], axis=0)
        local(send5, recv5.at[my_chunk], recv_sem.at[4]).start()

        def send(i):
            other = lax.rem(me * cores + core + i + 1, devices)
            remote(send5, recv5.at[my_chunk], 4, other // cores, lax.rem(other, cores)).start()

        repeat(devices - 1, send)

    when_owner(gather_out)
    wait_bytes(recv5, recv_sem.at[4])
    for c in range(chunks):
        out[:, c * HD : (c + 1) * HD] = recv5[c]

    def owner_sends():
        wait_bytes(send1.at[pl.ds(0, heads - 1)], send_sem.at[0])
        wait_bytes(recv1.at[pl.ds(0, n - 1)], send_sem.at[1])
        wait_bytes(send4.at[pl.ds(0, chunks - 1)], send_sem.at[3])
        wait_bytes(recv4.at[pl.ds(0, devices - 1)], send_sem.at[4])

    when_owner(owner_sends)
    if spread > 1:

        @pl.when(jnp.logical_not(owner))
        def _():
            wait_bytes(send1, send_sem.at[0])
            wait_bytes(send4, send_sem.at[3])

    wait_bytes(recv3.at[pl.ds(0, n - 1)], send_sem.at[2])


def body(
    n,
    cores,
    hidden_state,
    query_weight,
    up_key,
    up_value,
    latent_key,
    latent_value,
    lengths,
    block_mask,
    out_weight,
):
    batch, context_len, _, rank = latent_key.shape
    width = query_weight.shape[2]
    heads = KPG * REP
    model = out_weight.shape[2]
    chunks = model // HD
    f32, bf16 = jnp.float32, jnp.bfloat16
    vmem = pltpu.VMEM
    return pl.pallas_call(
        functools.partial(kernel, n, cores),
        out_shape=jax.ShapeDtypeStruct((batch, model), f32),
        in_specs=[pl.BlockSpec(memory_space=pltpu.SMEM)] * 2
        + [pl.BlockSpec(memory_space=pltpu.VMEM)]
        + [pl.BlockSpec(memory_space=pl.ANY)] * 6,
        out_specs=pl.BlockSpec(memory_space=pltpu.VMEM),
        scratch_shapes=[
            vmem((max(query_weight.shape[0], HD), width), bf16),
            vmem(up_key.shape[1:], bf16),
            vmem(up_value.shape[1:], bf16),
            vmem((batch, context_len, rank), bf16),
            vmem((batch, context_len, rank), bf16),
            vmem((max(out_weight.shape[1], HD), model), bf16),
            vmem((heads, batch, HD), f32),
            vmem((n, batch, HD), f32),
            vmem((batch, HD), f32),
            vmem((heads, batch, HD), f32),
            vmem((rank // HD, heads * batch, HD), f32),
            vmem((rank // HD, heads * batch, HD), f32),
            vmem((heads * batch, HD), f32),
            vmem((heads, 2 * batch, HD), f32),
            vmem((n, 2 * batch, HD), f32),
            vmem((chunks, batch, HD), f32),
            vmem((n * cores, batch, HD), f32),
            vmem((batch, HD), f32),
            vmem((chunks, batch, HD), f32),
            pltpu.SemaphoreType.DMA((4,)),
            pltpu.SemaphoreType.DMA((batch,)),
            pltpu.SemaphoreType.DMA((batch,)),
            pltpu.SemaphoreType.DMA((5,)),
            pltpu.SemaphoreType.DMA((5,)),
        ],
        compiler_params=pltpu.CompilerParams(collective_id=0, has_side_effects=True),
    )(
        lengths,
        block_mask.T,
        hidden_state,
        query_weight.reshape(query_weight.shape[0], width),
        up_key.reshape(up_key.shape[1:]),
        up_value.reshape(up_value.shape[1:]),
        latent_key.reshape(batch, context_len, rank),
        latent_value.reshape(batch, context_len, rank),
        out_weight.reshape(out_weight.shape[1:]),
    )


def solution(mesh):
    in_specs = (
        P(),
        P("seq", "head", None),
        P("head", None, None),
        P("head", None, None),
        P(None, "seq", "head", None),
        P(None, "seq", "head", None),
        P(),
        P(None, "seq"),
        P("head", "seq", None),
    )
    return jax.shard_map(
        functools.partial(body, mesh.shape["seq"], mesh.shape["head"]),
        mesh=mesh,
        in_specs=in_specs,
        out_specs=P(),
        check_vma=False,
    )
```

```python
import functools
import math

import jax
import jax.numpy as jnp
from jax import lax
from jax.experimental import pallas as pl
from jax.experimental.pallas import tpu as pltpu
from jax.sharding import PartitionSpec as P

HD = 128
BLOCK = 256
KPG = 4
REP = 4
MESH = pl.DeviceIdType.MESH
NEG = -1e30


def each_other(me, count, step):
    if count <= 32 and count & (count - 1) == 0:
        flips = [(1 << b) * (1 - 2 * lax.rem(me // (1 << b), 2)) for b in range(count.bit_length() - 1)]
        for mask in reversed(range(1, count)):
            step(me + sum(flip for b, flip in enumerate(flips) if mask >> b & 1))
    else:
        lax.fori_loop(0, count - 1, lambda i, c: (step(lax.rem(me + i + 1, count)), c)[1], 0)


def halves(x):
    high = x.astype(jnp.bfloat16)
    low = (x - high.astype(jnp.float32)).astype(jnp.bfloat16)
    return jnp.concatenate([high, low], axis=0)


def dot_nt(a, b):
    return lax.dot_general(a, b, (((1,), (1,)), ((), ())), preferred_element_type=jnp.float32)


def strided(ref, first, count, stride):
    parts = [ref[k, pl.ds(first, count, stride=stride), :] for k in range(ref.shape[0])]
    return jnp.concatenate(parts, axis=1)


def folded(x):
    rows = x.shape[0] // 2
    return x[:rows] + x[rows:]


def kernel(
    n,
    cores,
    lengths_in,
    mask_in,
    hidden_in,
    query_weight,
    up_key,
    up_value,
    keys,
    values,
    out_weight,
    out,
    lengths,
    block_mask,
    hidden,
    qw,
    uk,
    uv,
    kv,
    vv,
    ow,
    send1,
    recv1,
    send2,
    recv2,
    ql,
    ls,
    st,
    send3,
    recv3,
    send4,
    recv4,
    send5,
    recv5,
    send6,
    recv6,
    send7,
    recv7,
    pw,
    load_sem,
    key_sem,
    value_sem,
    send_sem,
    recv_sem,
):
    me = lax.axis_index("seq")
    core = lax.axis_index("head")
    batch, context_len = keys.shape[0], keys.shape[1]
    heads = KPG * REP
    spread = n // heads
    my_head = me // spread
    chunks = out.shape[1] // HD
    my_chunk = core * heads + my_head
    dim_rows, out_rows = query_weight.shape[0], out_weight.shape[0]
    owner = lax.rem(me, spread) == 0

    def local(src, dst, sem):
        return pltpu.make_async_copy(src, dst, sem)

    def remote(src, dst, phase, seq, head):
        return pltpu.make_async_remote_copy(
            src_ref=src,
            dst_ref=dst,
            send_sem=send_sem.at[phase],
            recv_sem=recv_sem.at[phase],
            device_id=(seq, head),
            device_id_type=MESH,
        )

    def to_either(here, src, dst, phase, seq, head):
        if here is True:
            local(src, dst, recv_sem.at[phase]).start()
        elif here is False:
            remote(src, dst, phase, seq, head).start()
        else:

            @pl.when(here)
            def _():
                local(src, dst, recv_sem.at[phase]).start()

            @pl.when(jnp.logical_not(here))
            def _():
                remote(src, dst, phase, seq, head).start()

    def wait_bytes(ref, sem):
        local(ref, ref, sem).wait()

    def when_owner(action):
        if spread == 1:
            action()
        else:
            pl.when(owner)(action)

    def first_is_here():
        return True if spread == 1 else owner

    if dim_rows >= HD:
        qw_at = qw
    else:
        qw_at = qw.at[pl.ds(pl.multiple_of(lax.rem(me * dim_rows, HD), dim_rows), dim_rows)]
    qw_copy = local(query_weight, qw_at, load_sem.at[0])
    hidden_copy = local(hidden_in, hidden, load_sem.at[4])
    hidden_copy.start()
    qw_copy.start()

    barrier = pltpu.get_barrier_semaphore()
    devices = n * cores

    def greet(other):
        pl.semaphore_signal(
            barrier, inc=1, device_id=(other // cores, lax.rem(other, cores)), device_id_type=MESH
        )

    each_other(me * cores + core, devices, greet)

    hidden_copy.wait()
    qw_copy.wait()
    lengths_copy = local(lengths_in, lengths, load_sem.at[5])
    lengths_copy.start()
    mask_copy = local(mask_in, block_mask, load_sem.at[6])
    mask_copy.start()
    uk_copy = local(up_key, uk, load_sem.at[1])
    uk_copy.start()
    key_copies = [local(keys.at[b], kv.at[b], key_sem.at[b]) for b in range(batch)]
    value_copies = [local(values.at[b], vv.at[b], value_sem.at[b]) for b in range(batch)]
    for b in range(batch):
        key_copies[b].start()
        value_copies[b].start()
    uv_copy = local(up_value, uv, load_sem.at[2])
    uv_copy.start()
    if out_rows >= HD:
        ow_at = ow
    else:
        ow_at = ow.at[pl.ds(pl.multiple_of(lax.rem(me * out_rows, HD), out_rows), out_rows)]
    ow_copy = local(out_weight, ow_at, load_sem.at[3])
    ow_copy.start()

    if dim_rows >= HD:
        state = hidden[:, pl.ds(pl.multiple_of(me * dim_rows, HD), dim_rows)]
        weight = qw[...]
    else:
        start = lax.rem(me * dim_rows, HD)
        state = hidden[:, pl.ds(pl.multiple_of(me * dim_rows - start, HD), HD)]
        row = lax.broadcasted_iota(jnp.int32, qw.shape, 0)
        weight = jnp.where((row >= start) & (row < start + dim_rows), qw[...].astype(jnp.float32), 0.0)
        weight = weight.astype(jnp.bfloat16)
    part = jnp.dot(state, weight, preferred_element_type=jnp.float32)
    for h in range(heads):
        send1[h] = part[:, h * HD : (h + 1) * HD]

    pl.semaphore_wait(barrier, devices - 1)

    def send_query(h):
        remote(send1.at[h], recv1.at[me], 0, h * spread, core).start()

    each_other(my_head, heads, send_query)
    to_either(first_is_here(), send1.at[my_head], recv1.at[me], 0, my_head * spread, core)

    def gather_query():
        wait_bytes(recv1, recv_sem.at[0])
        send2[...] = jnp.sum(recv1[...], axis=0)

        def send(other):
            remote(send2, recv2.at[my_head], 1, other, core).start()

        each_other(me, n, send)
        local(send2, recv2.at[my_head], recv_sem.at[1]).start()

    when_owner(gather_query)
    uk_copy.wait()
    wait_bytes(recv2, recv_sem.at[1])

    scale = 1.0 / math.sqrt(HD)
    rank = uk.shape[0]
    for j in range(KPG):
        rows = recv2[j * REP : (j + 1) * REP].reshape(REP * batch, HD)
        mapped = folded(dot_nt(halves(rows), uk[:, j * HD : (j + 1) * HD])) * scale
        for k in range(rank // HD):
            ql[k, j * REP * batch : (j + 1) * REP * batch, :] = mapped[:, k * HD : (k + 1) * HD]

    lengths_copy.wait()
    mask_copy.wait()
    blocks = context_len // BLOCK
    lane = lax.broadcasted_iota(jnp.int32, (1, BLOCK), 1)
    stat_lane = lax.broadcasted_iota(jnp.int32, (heads, HD), 1)
    for b in range(batch):
        key_copies[b].wait()
    for b in range(batch):
        query = halves(strided(ql, b, heads, batch))
        scores = folded(dot_nt(query, kv[b]))
        limits = [
            jnp.where(block_mask[k, b] == 1, lengths[b] - me * context_len - k * BLOCK, 0)
            for k in range(blocks)
        ]
        valid = jnp.concatenate([lane < limit for limit in limits], axis=1)
        scores = jnp.where(valid, scores, NEG)
        peak = jnp.max(scores, axis=1, keepdims=True)
        weights = jnp.where(valid, jnp.exp(scores - peak), 0.0)
        total = jnp.sum(weights, axis=1, keepdims=True)
        pw[b] = halves(weights)
        st[b * heads : (b + 1) * heads, :] = jnp.where(stat_lane < HD // 2, peak, total)
    for h in range(heads):
        send6[h] = st[pl.ds(h, batch, stride=heads), :]

    def send_stats(other):
        remote(send6.at[other // spread], recv6.at[me], 5, other, core).start()

    each_other(me, n, send_stats)
    local(send6.at[my_head], recv6.at[me], recv_sem.at[5]).start()

    for b in range(batch):
        value_copies[b].wait()
    for b in range(batch):
        latent = folded(jnp.dot(pw[b], vv[b], preferred_element_type=jnp.float32))
        for k in range(rank // HD):
            ls[k, b * heads : (b + 1) * heads, :] = latent[:, k * HD : (k + 1) * HD]

    uv_copy.wait()
    for j in range(KPG):
        rows = jnp.concatenate(
            [strided(ls, j * REP + r, batch, heads) for r in range(REP)], axis=0
        )
        summed = folded(
            jnp.dot(halves(rows), uv[:, j * HD : (j + 1) * HD], preferred_element_type=jnp.float32)
        )
        for r in range(REP):
            h = j * REP + r
            send3[h] = summed[r * batch : (r + 1) * batch]

    def send_carry(other):
        remote(send3.at[other // spread], recv3.at[me], 2, other, core).start()

    each_other(me, n, send_carry)
    local(send3.at[my_head], recv3.at[me], recv_sem.at[2]).start()

    wait_bytes(recv6, recv_sem.at[5])
    stats = recv6[...]
    turned = pltpu.roll(stats, HD // 2, 2)
    low_lanes = lax.broadcasted_iota(jnp.int32, stats.shape, 2) < HD // 2
    peaks = jnp.where(low_lanes, stats, turned)
    totals = jnp.where(low_lanes, turned, stats)
    factor = jnp.exp(peaks - jnp.max(peaks, axis=0, keepdims=True))
    factor = factor / jnp.sum(totals * factor, axis=0, keepdims=True)

    wait_bytes(recv3, recv_sem.at[2])

    context = jnp.sum(recv3[...] * factor, axis=0).astype(jnp.bfloat16)

    ow_copy.wait()
    if out_rows >= HD:
        weight = ow[...]
    else:
        start = lax.rem(me * out_rows, HD)
        row = lax.broadcasted_iota(jnp.int32, ow.shape, 0)
        weight = jnp.where((row >= start) & (row < start + out_rows), ow[...].astype(jnp.float32), 0.0)
        weight = weight.astype(jnp.bfloat16)
    part = jnp.dot(context, weight, preferred_element_type=jnp.float32)
    for c in range(chunks):
        send4[c] = part[:, c * HD : (c + 1) * HD]

    half = chunks // cores
    remote(send4.at[pl.ds((1 - core) * half, half)], recv7, 6, me, 1 - core).start()
    wait_bytes(recv7, recv_sem.at[6])
    send7[...] = send4[pl.ds(core * half, half)] + recv7[...]

    def send_part(c):
        remote(send7.at[c], recv4.at[me], 3, c * spread, core).start()

    each_other(my_head, heads, send_part)
    to_either(first_is_here(), send7.at[my_head], recv4.at[me], 3, my_head * spread, core)

    def gather_out():
        wait_bytes(recv4, recv_sem.at[3])
        send5[...] = jnp.sum(recv4[...], axis=0)

        def send(other):
            remote(send5, recv5.at[my_chunk], 4, other // cores, lax.rem(other, cores)).start()

        each_other(me * cores + core, devices, send)
        local(send5, recv5.at[my_chunk], recv_sem.at[4]).start()

    when_owner(gather_out)
    wait_bytes(recv5, recv_sem.at[4])
    for c in range(chunks):
        out[:, c * HD : (c + 1) * HD] = recv5[c]

    def owner_sends():
        wait_bytes(send1.at[pl.ds(0, heads - 1)], send_sem.at[0])
        wait_bytes(recv1.at[pl.ds(0, n - 1)], send_sem.at[1])
        wait_bytes(send7.at[pl.ds(0, heads - 1)], send_sem.at[3])
        if devices - 1 <= chunks:
            wait_bytes(recv5.at[pl.ds(0, devices - 1)], send_sem.at[4])
        else:
            wait_bytes(recv4, send_sem.at[4])
            wait_bytes(recv4.at[pl.ds(0, n - 1)], send_sem.at[4])

    when_owner(owner_sends)
    if spread > 1:

        @pl.when(jnp.logical_not(owner))
        def _():
            wait_bytes(send1, send_sem.at[0])
            wait_bytes(send7, send_sem.at[3])

    wait_bytes(recv3.at[pl.ds(0, n - 1)], send_sem.at[2])
    wait_bytes(recv6.at[pl.ds(0, n - 1)], send_sem.at[5])
    wait_bytes(recv7, send_sem.at[6])


def body(
    n,
    cores,
    hidden_state,
    query_weight,
    up_key,
    up_value,
    latent_key,
    latent_value,
    lengths,
    block_mask,
    out_weight,
):
    batch, context_len, _, rank = latent_key.shape
    width = query_weight.shape[2]
    heads = KPG * REP
    model = out_weight.shape[2]
    chunks = model // HD
    f32, bf16 = jnp.float32, jnp.bfloat16
    vmem = pltpu.VMEM
    return pl.pallas_call(
        functools.partial(kernel, n, cores),
        out_shape=jax.ShapeDtypeStruct((batch, model), f32),
        in_specs=[pl.BlockSpec(memory_space=pl.ANY)] * 9,
        out_specs=pl.BlockSpec(memory_space=pltpu.VMEM),
        scratch_shapes=[
            pltpu.SMEM(lengths.shape, jnp.int32),
            pltpu.SMEM(block_mask.shape[::-1], jnp.int32),
            vmem(hidden_state.shape, bf16),
            vmem((max(query_weight.shape[0], HD), width), bf16),
            vmem(up_key.shape[1:], bf16),
            vmem(up_value.shape[1:], bf16),
            vmem((batch, context_len, rank), bf16),
            vmem((batch, context_len, rank), bf16),
            vmem((max(out_weight.shape[1], HD), model), bf16),
            vmem((heads, batch, HD), f32),
            vmem((n, batch, HD), f32),
            vmem((batch, HD), f32),
            vmem((heads, batch, HD), f32),
            vmem((rank // HD, heads * batch, HD), f32),
            vmem((rank // HD, heads * batch, HD), f32),
            vmem((heads * batch, HD), f32),
            vmem((heads, batch, HD), f32),
            vmem((n, batch, HD), f32),
            vmem((chunks, batch, HD), f32),
            vmem((n, batch, HD), f32),
            vmem((batch, HD), f32),
            vmem((chunks, batch, HD), f32),
            vmem((heads, batch, HD), f32),
            vmem((n, batch, HD), f32),
            vmem((chunks // cores, batch, HD), f32),
            vmem((chunks // cores, batch, HD), f32),
            vmem((batch, 2 * heads, context_len), bf16),
            pltpu.SemaphoreType.DMA((7,)),
            pltpu.SemaphoreType.DMA((batch,)),
            pltpu.SemaphoreType.DMA((batch,)),
            pltpu.SemaphoreType.DMA((7,)),
            pltpu.SemaphoreType.DMA((7,)),
        ],
        compiler_params=pltpu.CompilerParams(collective_id=0, has_side_effects=True),
    )(
        lengths,
        block_mask.T,
        hidden_state,
        query_weight.reshape(query_weight.shape[0], width),
        up_key.reshape(up_key.shape[1:]),
        up_value.reshape(up_value.shape[1:]),
        latent_key.reshape(batch, context_len, rank),
        latent_value.reshape(batch, context_len, rank),
        out_weight.reshape(out_weight.shape[1:]),
    )


def solution(mesh):
    in_specs = (
        P(),
        P("seq", "head", None),
        P("head", None, None),
        P("head", None, None),
        P(None, "seq", "head", None),
        P(None, "seq", "head", None),
        P(),
        P(None, "seq"),
        P("head", "seq", None),
    )
    return jax.shard_map(
        functools.partial(body, mesh.shape["seq"], mesh.shape["head"]),
        mesh=mesh,
        in_specs=in_specs,
        out_specs=P(),
        check_vma=False,
    )
```

```python
import functools
import math

import jax
import jax.numpy as jnp
from jax import lax
from jax.experimental import pallas as pl
from jax.experimental.pallas import tpu as pltpu
from jax.sharding import PartitionSpec as P

HD = 128
BLOCK = 256
KPG = 4
REP = 4
MESH = pl.DeviceIdType.MESH
NEG = -1e30


def each_other(me, count, step):
    if count <= 32 and count & (count - 1) == 0:
        flips = [(1 << b) * (1 - 2 * lax.rem(me // (1 << b), 2)) for b in range(count.bit_length() - 1)]
        for mask in reversed(range(1, count)):
            step(me + sum(flip for b, flip in enumerate(flips) if mask >> b & 1))
    else:
        lax.fori_loop(0, count - 1, lambda i, c: (step(lax.rem(me + i + 1, count)), c)[1], 0)


def halves(x):
    high = x.astype(jnp.bfloat16)
    low = (x - high.astype(jnp.float32)).astype(jnp.bfloat16)
    return jnp.concatenate([high, low], axis=0)


def dot_nt(a, b):
    return lax.dot_general(a, b, (((1,), (1,)), ((), ())), preferred_element_type=jnp.float32)


def strided(ref, first, count, stride):
    parts = [ref[k, pl.ds(first, count, stride=stride), :] for k in range(ref.shape[0])]
    return jnp.concatenate(parts, axis=1)


def folded(x):
    rows = x.shape[0] // 2
    return x[:rows] + x[rows:]


def kernel(
    n,
    cores,
    lengths_in,
    mask_in,
    hidden_in,
    query_weight,
    up_key,
    up_value,
    keys,
    values,
    out_weight,
    out,
    lengths,
    block_mask,
    hidden,
    qw,
    uk,
    uv,
    kv,
    vv,
    ow,
    send1,
    recv1,
    send2,
    recv2,
    ql,
    ls,
    st,
    send3,
    recv3,
    send4,
    recv4,
    send5,
    recv5,
    send6,
    recv6,
    send7,
    recv7,
    pw,
    load_sem,
    key_sem,
    value_sem,
    send_sem,
    recv_sem,
):
    me = lax.axis_index("seq")
    core = lax.axis_index("head")
    batch, context_len = keys.shape[0], keys.shape[1]
    heads = KPG * REP
    spread = n // heads
    my_head = me // spread
    chunks = out.shape[1] // HD
    my_chunk = core * heads + my_head
    dim_rows, out_rows = query_weight.shape[0], out_weight.shape[0]
    owner = lax.rem(me, spread) == 0

    def local(src, dst, sem):
        return pltpu.make_async_copy(src, dst, sem)

    def remote(src, dst, phase, seq, head):
        return pltpu.make_async_remote_copy(
            src_ref=src,
            dst_ref=dst,
            send_sem=send_sem.at[phase],
            recv_sem=recv_sem.at[phase],
            device_id=(seq, head),
            device_id_type=MESH,
        )

    def to_either(here, src, dst, phase, seq, head):
        if here is True:
            local(src, dst, recv_sem.at[phase]).start()
        elif here is False:
            remote(src, dst, phase, seq, head).start()
        else:

            @pl.when(here)
            def _():
                local(src, dst, recv_sem.at[phase]).start()

            @pl.when(jnp.logical_not(here))
            def _():
                remote(src, dst, phase, seq, head).start()

    def wait_bytes(ref, sem):
        local(ref, ref, sem).wait()

    def when_owner(action):
        if spread == 1:
            action()
        else:
            pl.when(owner)(action)

    def first_is_here():
        return True if spread == 1 else owner

    if dim_rows >= HD:
        qw_at = qw
    else:
        qw_at = qw.at[pl.ds(pl.multiple_of(lax.rem(me * dim_rows, HD), dim_rows), dim_rows)]
    qw_copy = local(query_weight, qw_at, load_sem.at[0])
    hidden_copy = local(hidden_in, hidden, load_sem.at[4])
    hidden_copy.start()
    qw_copy.start()

    barrier = pltpu.get_barrier_semaphore()
    devices = n * cores

    def greet(other):
        pl.semaphore_signal(
            barrier, inc=1, device_id=(other // cores, lax.rem(other, cores)), device_id_type=MESH
        )

    each_other(me * cores + core, devices, greet)

    hidden_copy.wait()
    qw_copy.wait()
    lengths_copy = local(lengths_in, lengths, load_sem.at[5])
    lengths_copy.start()
    mask_copy = local(mask_in, block_mask, load_sem.at[6])
    mask_copy.start()
    uk_copy = local(up_key, uk, load_sem.at[1])
    uk_copy.start()
    key_copies = [local(keys.at[b], kv.at[b], key_sem.at[b]) for b in range(batch)]
    value_copies = [local(values.at[b], vv.at[b], value_sem.at[b]) for b in range(batch)]
    for b in range(batch):
        key_copies[b].start()
        value_copies[b].start()
    uv_copy = local(up_value, uv, load_sem.at[2])
    uv_copy.start()
    if out_rows >= HD:
        ow_at = ow
    else:
        ow_at = ow.at[pl.ds(pl.multiple_of(lax.rem(me * out_rows, HD), out_rows), out_rows)]
    ow_copy = local(out_weight, ow_at, load_sem.at[3])
    ow_copy.start()

    if dim_rows >= HD:
        state = hidden[:, pl.ds(pl.multiple_of(me * dim_rows, HD), dim_rows)]
        weight = qw[...]
    else:
        start = lax.rem(me * dim_rows, HD)
        state = hidden[:, pl.ds(pl.multiple_of(me * dim_rows - start, HD), HD)]
        row = lax.broadcasted_iota(jnp.int32, qw.shape, 0)
        weight = jnp.where((row >= start) & (row < start + dim_rows), qw[...].astype(jnp.float32), 0.0)
        weight = weight.astype(jnp.bfloat16)
    part = jnp.dot(state, weight, preferred_element_type=jnp.float32)
    for h in range(heads):
        send1[h] = part[:, h * HD : (h + 1) * HD]

    pl.semaphore_wait(barrier, devices - 1)

    def send_query(h):
        remote(send1.at[h], recv1.at[me], 0, h * spread, core).start()

    each_other(my_head, heads, send_query)
    to_either(first_is_here(), send1.at[my_head], recv1.at[me], 0, my_head * spread, core)

    def gather_query():
        wait_bytes(recv1, recv_sem.at[0])
        send2[...] = jnp.sum(recv1[...], axis=0)

        def send(other):
            remote(send2, recv2.at[my_head], 1, other, core).start()

        each_other(me, n, send)
        local(send2, recv2.at[my_head], recv_sem.at[1]).start()

    when_owner(gather_query)
    uk_copy.wait()
    wait_bytes(recv2, recv_sem.at[1])

    scale = 1.0 / math.sqrt(HD)
    rank = uk.shape[0]
    for j in range(KPG):
        rows = recv2[j * REP : (j + 1) * REP].reshape(REP * batch, HD)
        mapped = folded(dot_nt(halves(rows), uk[:, j * HD : (j + 1) * HD])) * scale
        for k in range(rank // HD):
            ql[k, j * REP * batch : (j + 1) * REP * batch, :] = mapped[:, k * HD : (k + 1) * HD]

    lengths_copy.wait()
    mask_copy.wait()
    blocks = context_len // BLOCK
    lane = lax.broadcasted_iota(jnp.int32, (1, BLOCK), 1)
    stat_lane = lax.broadcasted_iota(jnp.int32, (heads, HD), 1)
    for b in range(batch):
        key_copies[b].wait()
    for b in range(batch):
        query = halves(strided(ql, b, heads, batch))
        scores = folded(dot_nt(query, kv[b]))
        limits = [
            jnp.where(block_mask[k, b] == 1, lengths[b] - me * context_len - k * BLOCK, 0)
            for k in range(blocks)
        ]
        valid = jnp.concatenate([lane < limit for limit in limits], axis=1)
        scores = jnp.where(valid, scores, NEG)
        peak = jnp.max(scores, axis=1, keepdims=True)
        weights = jnp.where(valid, jnp.exp(scores - peak), 0.0)
        total = jnp.sum(weights, axis=1, keepdims=True)
        pw[b] = halves(weights)
        st[b * heads : (b + 1) * heads, :] = jnp.where(stat_lane < HD // 2, peak, total)
    for h in range(heads):
        send6[h] = st[pl.ds(h, batch, stride=heads), :]

    def send_stats(other):
        remote(send6.at[other // spread], recv6.at[me], 5, other, core).start()

    each_other(me, n, send_stats)
    local(send6.at[my_head], recv6.at[me], recv_sem.at[5]).start()

    for b in range(batch):
        value_copies[b].wait()
    for b in range(batch):
        latent = folded(jnp.dot(pw[b], vv[b], preferred_element_type=jnp.float32))
        for k in range(rank // HD):
            ls[k, b * heads : (b + 1) * heads, :] = latent[:, k * HD : (k + 1) * HD]

    uv_copy.wait()
    for j in range(KPG):
        rows = jnp.concatenate(
            [strided(ls, j * REP + r, batch, heads) for r in range(REP)], axis=0
        )
        summed = folded(
            jnp.dot(halves(rows), uv[:, j * HD : (j + 1) * HD], preferred_element_type=jnp.float32)
        )
        for r in range(REP):
            h = j * REP + r
            send3[h] = summed[r * batch : (r + 1) * batch]

    def send_carry(other):
        remote(send3.at[other // spread], recv3.at[me], 2, other, core).start()

    each_other(me, n, send_carry)
    local(send3.at[my_head], recv3.at[me], recv_sem.at[2]).start()

    wait_bytes(recv6, recv_sem.at[5])
    stats = recv6[...]
    turned = pltpu.roll(stats, HD // 2, 2)
    low_lanes = lax.broadcasted_iota(jnp.int32, stats.shape, 2) < HD // 2
    peaks = jnp.where(low_lanes, stats, turned)
    totals = jnp.where(low_lanes, turned, stats)
    factor = jnp.exp(peaks - jnp.max(peaks, axis=0, keepdims=True))
    factor = factor / jnp.sum(totals * factor, axis=0, keepdims=True)

    wait_bytes(recv3, recv_sem.at[2])

    context = jnp.sum(recv3[...] * factor, axis=0).astype(jnp.bfloat16)

    ow_copy.wait()
    if out_rows >= HD:
        weight = ow[...]
    else:
        start = lax.rem(me * out_rows, HD)
        row = lax.broadcasted_iota(jnp.int32, ow.shape, 0)
        weight = jnp.where((row >= start) & (row < start + out_rows), ow[...].astype(jnp.float32), 0.0)
        weight = weight.astype(jnp.bfloat16)
    part = jnp.dot(context, weight, preferred_element_type=jnp.float32)
    for c in range(chunks):
        send4[c] = part[:, c * HD : (c + 1) * HD]

    half = chunks // cores
    remote(send4.at[pl.ds((1 - core) * half, half)], recv7, 6, me, 1 - core).start()
    wait_bytes(recv7, recv_sem.at[6])
    send7[...] = send4[pl.ds(core * half, half)] + recv7[...]

    def send_part(c):
        remote(send7.at[c], recv4.at[me], 3, c * spread, core).start()

    each_other(my_head, heads, send_part)
    to_either(first_is_here(), send7.at[my_head], recv4.at[me], 3, my_head * spread, core)

    def gather_out():
        wait_bytes(recv4, recv_sem.at[3])
        send5[...] = jnp.sum(recv4[...], axis=0)

        def send(other):
            remote(send5, recv5.at[my_chunk], 4, other // cores, lax.rem(other, cores)).start()

        each_other(me * cores + core, devices, send)
        local(send5, recv5.at[my_chunk], recv_sem.at[4]).start()

    when_owner(gather_out)
    wait_bytes(recv5, recv_sem.at[4])
    for c in range(chunks):
        out[:, c * HD : (c + 1) * HD] = recv5[c]

    def owner_sends():
        wait_bytes(send1.at[pl.ds(0, heads - 1)], send_sem.at[0])
        wait_bytes(recv1.at[pl.ds(0, n - 1)], send_sem.at[1])
        wait_bytes(send7.at[pl.ds(0, heads - 1)], send_sem.at[3])
        if devices - 1 <= chunks:
            wait_bytes(recv5.at[pl.ds(0, devices - 1)], send_sem.at[4])
        else:
            wait_bytes(recv4, send_sem.at[4])
            wait_bytes(recv4.at[pl.ds(0, n - 1)], send_sem.at[4])

    when_owner(owner_sends)
    if spread > 1:

        @pl.when(jnp.logical_not(owner))
        def _():
            wait_bytes(send1, send_sem.at[0])
            wait_bytes(send7, send_sem.at[3])

    wait_bytes(recv3.at[pl.ds(0, n - 1)], send_sem.at[2])
    wait_bytes(recv6.at[pl.ds(0, n - 1)], send_sem.at[5])
    wait_bytes(recv7, send_sem.at[6])


def body(
    n,
    cores,
    hidden_state,
    query_weight,
    up_key,
    up_value,
    latent_key,
    latent_value,
    lengths,
    block_mask,
    out_weight,
):
    batch, context_len, _, rank = latent_key.shape
    width = query_weight.shape[2]
    heads = KPG * REP
    model = out_weight.shape[2]
    chunks = model // HD
    f32, bf16 = jnp.float32, jnp.bfloat16
    vmem = pltpu.VMEM
    return pl.pallas_call(
        functools.partial(kernel, n, cores),
        out_shape=pltpu.VMEM((batch, model), f32),
        in_specs=[pl.BlockSpec(memory_space=pl.ANY)] * 9,
        out_specs=pl.BlockSpec(memory_space=pltpu.VMEM),
        scratch_shapes=[
            pltpu.SMEM(lengths.shape, jnp.int32),
            pltpu.SMEM(block_mask.shape[::-1], jnp.int32),
            vmem(hidden_state.shape, bf16),
            vmem((max(query_weight.shape[0], HD), width), bf16),
            vmem(up_key.shape[1:], bf16),
            vmem(up_value.shape[1:], bf16),
            vmem((batch, context_len, rank), bf16),
            vmem((batch, context_len, rank), bf16),
            vmem((max(out_weight.shape[1], HD), model), bf16),
            vmem((heads, batch, HD), f32),
            vmem((n, batch, HD), f32),
            vmem((batch, HD), f32),
            vmem((heads, batch, HD), f32),
            vmem((rank // HD, heads * batch, HD), f32),
            vmem((rank // HD, heads * batch, HD), f32),
            vmem((heads * batch, HD), f32),
            vmem((heads, batch, HD), f32),
            vmem((n, batch, HD), f32),
            vmem((chunks, batch, HD), f32),
            vmem((n, batch, HD), f32),
            vmem((batch, HD), f32),
            vmem((chunks, batch, HD), f32),
            vmem((heads, batch, HD), f32),
            vmem((n, batch, HD), f32),
            vmem((chunks // cores, batch, HD), f32),
            vmem((chunks // cores, batch, HD), f32),
            vmem((batch, 2 * heads, context_len), bf16),
            pltpu.SemaphoreType.DMA((7,)),
            pltpu.SemaphoreType.DMA((batch,)),
            pltpu.SemaphoreType.DMA((batch,)),
            pltpu.SemaphoreType.DMA((7,)),
            pltpu.SemaphoreType.DMA((7,)),
        ],
        compiler_params=pltpu.CompilerParams(collective_id=0, has_side_effects=True),
    )(
        lengths,
        block_mask.T,
        hidden_state,
        query_weight.reshape(query_weight.shape[0], width),
        up_key.reshape(up_key.shape[1:]),
        up_value.reshape(up_value.shape[1:]),
        latent_key.reshape(batch, context_len, rank),
        latent_value.reshape(batch, context_len, rank),
        out_weight.reshape(out_weight.shape[1:]),
    )


def solution(mesh):
    in_specs = (
        P(),
        P("seq", "head", None),
        P("head", None, None),
        P("head", None, None),
        P(None, "seq", "head", None),
        P(None, "seq", "head", None),
        P(),
        P(None, "seq"),
        P("head", "seq", None),
    )
    return jax.shard_map(
        functools.partial(body, mesh.shape["seq"], mesh.shape["head"]),
        mesh=mesh,
        in_specs=in_specs,
        out_specs=P(),
        check_vma=False,
    )
```

```python
import functools
import math

import jax
import jax.numpy as jnp
from jax import lax
from jax.experimental import pallas as pl
from jax.experimental.pallas import tpu as pltpu
from jax.sharding import PartitionSpec as P

HD = 128
BLOCK = 256
KPG = 4
REP = 4
MESH = pl.DeviceIdType.MESH
NEG = -1e30


def each_other(me, count, step):
    if count <= 32 and count & (count - 1) == 0:
        flips = [(1 << b) * (1 - 2 * lax.rem(me // (1 << b), 2)) for b in range(count.bit_length() - 1)]
        for mask in reversed(range(1, count)):
            step(me + sum(flip for b, flip in enumerate(flips) if mask >> b & 1))
    else:
        lax.fori_loop(0, count - 1, lambda i, c: (step(lax.rem(me + i + 1, count)), c)[1], 0)


def halves(x):
    high = x.astype(jnp.bfloat16)
    low = (x - high.astype(jnp.float32)).astype(jnp.bfloat16)
    return jnp.concatenate([high, low], axis=0)


def dot_nt(a, b):
    return lax.dot_general(a, b, (((1,), (1,)), ((), ())), preferred_element_type=jnp.float32)


def strided(ref, first, count, stride):
    parts = [ref[k, pl.ds(first, count, stride=stride), :] for k in range(ref.shape[0])]
    return jnp.concatenate(parts, axis=1)


def folded(x):
    rows = x.shape[0] // 2
    return x[:rows] + x[rows:]


def kernel(
    n,
    cores,
    lengths_in,
    mask_in,
    hidden_in,
    query_weight,
    up_key,
    up_value,
    keys,
    values,
    out_weight,
    out,
    lengths,
    block_mask,
    hidden,
    qw,
    uk,
    uv,
    kv,
    vv,
    ow,
    send1,
    recv1,
    send2,
    recv2,
    ql,
    ls,
    st,
    send3,
    recv3,
    send4,
    recv4,
    send5,
    recv5,
    send6,
    recv6,
    rows_out,
    rows_in,
    pw,
    load_sem,
    key_sem,
    value_sem,
    send_sem,
    recv_sem,
):
    me = lax.axis_index("seq")
    core = lax.axis_index("head")
    batch, context_len = keys.shape[0], keys.shape[1]
    heads = KPG * REP
    spread = n // heads
    my_head = me // spread
    per_head = out.shape[1] // HD // heads
    hub = cores - 1
    groups = recv1.shape[0]
    dim_rows, out_rows = query_weight.shape[0], out_weight.shape[0]
    owner = lax.rem(me, spread) == 0
    is_hub = core == hub

    def local(src, dst, sem):
        return pltpu.make_async_copy(src, dst, sem)

    def remote(src, dst, phase, seq, head):
        return pltpu.make_async_remote_copy(
            src_ref=src,
            dst_ref=dst,
            send_sem=send_sem.at[phase],
            recv_sem=recv_sem.at[phase],
            device_id=(seq, head),
            device_id_type=MESH,
        )

    def wait_bytes(ref, sem):
        local(ref, ref, sem).wait()

    def when_owner(action):
        pl.when(is_hub if spread == 1 else is_hub & owner)(action)

    def to_hub(other, own, src, dst, phase):
        if own is None:
            remote(src, dst, phase, other, hub).start()
        else:

            @pl.when(own)
            def _():
                local(src, dst, recv_sem.at[phase]).start()

            @pl.when(jnp.logical_not(own))
            def _():
                remote(src, dst, phase, other, hub).start()

    if dim_rows >= HD:
        qw_at = qw
    else:
        qw_at = qw.at[pl.ds(pl.multiple_of(lax.rem(me * dim_rows, HD), dim_rows), dim_rows)]
    qw_copy = local(query_weight, qw_at, load_sem.at[0])
    hidden_copy = local(hidden_in, hidden, load_sem.at[4])
    hidden_copy.start()
    qw_copy.start()

    def output_rows():
        if out_rows >= HD:
            return ow[...]
        start = lax.rem(me * out_rows, HD)
        row = lax.broadcasted_iota(jnp.int32, ow.shape, 0)
        kept = jnp.where((row >= start) & (row < start + out_rows), ow[...].astype(jnp.float32), 0.0)
        return kept.astype(jnp.bfloat16)

    barrier = pltpu.get_barrier_semaphore()
    devices = n * cores

    def greet(other):
        pl.semaphore_signal(
            barrier, inc=1, device_id=(other // cores, lax.rem(other, cores)), device_id_type=MESH
        )

    each_other(me * cores + core, devices, greet)

    hidden_copy.wait()
    qw_copy.wait()
    lengths_copy = local(lengths_in, lengths, load_sem.at[5])
    lengths_copy.start()
    mask_copy = local(mask_in, block_mask, load_sem.at[6])
    mask_copy.start()
    uk_copy = local(up_key, uk, load_sem.at[1])
    uk_copy.start()
    key_copies = [local(keys.at[b], kv.at[b], key_sem.at[b]) for b in range(batch)]
    value_copies = [local(values.at[b], vv.at[b], value_sem.at[b]) for b in range(batch)]
    for b in range(batch):
        key_copies[b].start()
        value_copies[b].start()
    uv_copy = local(up_value, uv, load_sem.at[2])
    uv_copy.start()
    if out_rows >= HD:
        ow_at = ow
    else:
        ow_at = ow.at[pl.ds(pl.multiple_of(lax.rem(me * out_rows, HD), out_rows), out_rows)]
    ow_copy = local(out_weight, ow_at, load_sem.at[3])
    ow_copy.start()

    if dim_rows >= HD:
        state = hidden[:, pl.ds(pl.multiple_of(me * dim_rows, HD), dim_rows)]
        weight = qw[...]
    else:
        start = lax.rem(me * dim_rows, HD)
        state = hidden[:, pl.ds(pl.multiple_of(me * dim_rows - start, HD), HD)]
        row = lax.broadcasted_iota(jnp.int32, qw.shape, 0)
        weight = jnp.where((row >= start) & (row < start + dim_rows), qw[...].astype(jnp.float32), 0.0)
        weight = weight.astype(jnp.bfloat16)
    part = jnp.dot(state, weight, preferred_element_type=jnp.float32)
    for h in range(heads):
        send1[h] = part[:, h * HD : (h + 1) * HD]

    pl.semaphore_wait(barrier, devices - 1)

    def send_query(h):
        to_hub(h * spread, None, send1.at[h], recv1.at[core, me], 0)

    each_other(my_head, heads, send_query)
    here = is_hub if spread == 1 else is_hub & owner
    to_hub(my_head * spread, here, send1.at[my_head], recv1.at[core, me], 0)

    ow_copy.wait()

    @pl.when(jnp.logical_not(is_hub))
    def _():
        rows_out[...] = output_rows().astype(jnp.float32)
        remote(rows_out, rows_in, 6, me, hub).start()

    def gather_query():
        wait_bytes(recv1, recv_sem.at[0])
        send2[...] = jnp.sum(recv1[...], axis=1)

        def send(other):
            for group in range(groups):
                remote(send2.at[group], recv2.at[my_head], 1, other, group).start()

        each_other(me, n, send)
        for group in range(groups - 1):
            remote(send2.at[group], recv2.at[my_head], 1, me, group).start()
        local(send2.at[hub], recv2.at[my_head], recv_sem.at[1]).start()

    when_owner(gather_query)
    uk_copy.wait()
    wait_bytes(recv2, recv_sem.at[1])

    scale = 1.0 / math.sqrt(HD)
    rank = uk.shape[0]
    for j in range(KPG):
        rows = recv2[j * REP : (j + 1) * REP].reshape(REP * batch, HD)
        mapped = folded(dot_nt(halves(rows), uk[:, j * HD : (j + 1) * HD])) * scale
        for k in range(rank // HD):
            ql[k, j * REP * batch : (j + 1) * REP * batch, :] = mapped[:, k * HD : (k + 1) * HD]

    lengths_copy.wait()
    mask_copy.wait()
    blocks = context_len // BLOCK
    lane = lax.broadcasted_iota(jnp.int32, (1, BLOCK), 1)
    stat_lane = lax.broadcasted_iota(jnp.int32, (heads, HD), 1)
    for b in range(batch):
        key_copies[b].wait()
    for b in range(batch):
        query = halves(strided(ql, b, heads, batch))
        scores = folded(dot_nt(query, kv[b]))
        limits = [
            jnp.where(block_mask[k, b] == 1, lengths[b] - me * context_len - k * BLOCK, 0)
            for k in range(blocks)
        ]
        valid = jnp.concatenate([lane < limit for limit in limits], axis=1)
        scores = jnp.where(valid, scores, NEG)
        peak = jnp.max(scores, axis=1, keepdims=True)
        weights = jnp.where(valid, jnp.exp(scores - peak), 0.0)
        total = jnp.sum(weights, axis=1, keepdims=True)
        pw[b] = halves(weights)
        st[b * heads : (b + 1) * heads, :] = jnp.where(stat_lane < HD // 2, peak, total)
    for h in range(heads):
        send6[h] = st[pl.ds(h, batch, stride=heads), :]

    def send_stats(other):
        to_hub(other, None, send6.at[other // spread], recv6.at[core, me], 5)

    each_other(me, n, send_stats)
    to_hub(me, is_hub, send6.at[my_head], recv6.at[core, me], 5)

    for b in range(batch):
        value_copies[b].wait()
    for b in range(batch):
        latent = folded(jnp.dot(pw[b], vv[b], preferred_element_type=jnp.float32))
        for k in range(rank // HD):
            ls[k, b * heads : (b + 1) * heads, :] = latent[:, k * HD : (k + 1) * HD]

    uv_copy.wait()
    for j in range(KPG):
        rows = jnp.concatenate(
            [strided(ls, j * REP + r, batch, heads) for r in range(REP)], axis=0
        )
        summed = folded(
            jnp.dot(halves(rows), uv[:, j * HD : (j + 1) * HD], preferred_element_type=jnp.float32)
        )
        for r in range(REP):
            h = j * REP + r
            send3[h] = summed[r * batch : (r + 1) * batch]

    def send_carry(other):
        to_hub(other, None, send3.at[other // spread], recv3.at[core, me], 2)

    each_other(me, n, send_carry)
    to_hub(me, is_hub, send3.at[my_head], recv3.at[core, me], 2)

    @pl.when(is_hub)
    def _():
        wait_bytes(rows_in, recv_sem.at[6])
        wait_bytes(recv6, recv_sem.at[5])
        stats = recv6[...]
        turned = pltpu.roll(stats, HD // 2, 3)
        low_lanes = lax.broadcasted_iota(jnp.int32, stats.shape, 3) < HD // 2
        peaks = jnp.where(low_lanes, stats, turned)
        totals = jnp.where(low_lanes, turned, stats)
        factor = jnp.exp(peaks - jnp.max(peaks, axis=1, keepdims=True))
        factor = factor / jnp.sum(totals * factor, axis=1, keepdims=True)
        rows = jnp.concatenate([rows_in[...].astype(jnp.bfloat16), output_rows()], axis=0)

        wait_bytes(recv3, recv_sem.at[2])
        context = jnp.sum(recv3[...] * factor, axis=1).astype(jnp.bfloat16)
        context = jnp.concatenate([context[group] for group in range(groups)], axis=1)
        part = jnp.dot(context, rows, preferred_element_type=jnp.float32)
        for c in range(heads * per_head):
            send4[c // per_head, c % per_head] = part[:, c * HD : (c + 1) * HD]

        def send_part(h):
            to_hub(h * spread, None, send4.at[h], recv4.at[me], 3)

        each_other(my_head, heads, send_part)
        here = None if spread == 1 else owner
        if here is None:
            local(send4.at[my_head], recv4.at[me], recv_sem.at[3]).start()
        else:
            to_hub(my_head * spread, here, send4.at[my_head], recv4.at[me], 3)

    def gather_out():
        wait_bytes(recv4, recv_sem.at[3])
        send5[...] = jnp.sum(recv4[...], axis=0)

        def send(other):
            for group in range(groups):
                remote(send5, recv5.at[my_head], 4, other, group).start()

        each_other(me, n, send)
        for group in range(groups - 1):
            remote(send5, recv5.at[my_head], 4, me, group).start()
        local(send5, recv5.at[my_head], recv_sem.at[4]).start()

    when_owner(gather_out)
    wait_bytes(recv5, recv_sem.at[4])
    for c in range(heads * per_head):
        out[:, c * HD : (c + 1) * HD] = recv5[c // per_head, c % per_head]

    for phase, piece in ((2, recv3), (5, recv6)):
        wait_bytes(piece.at[0, pl.ds(0, n - 1)], send_sem.at[phase])

        @pl.when(jnp.logical_not(is_hub))
        def _():
            wait_bytes(piece.at[0, 0], send_sem.at[phase])

    wait_bytes(send1.at[pl.ds(0, heads - 1)], send_sem.at[0])

    @pl.when(jnp.logical_not(here))
    def _():
        wait_bytes(send1.at[0], send_sem.at[0])

    @pl.when(jnp.logical_not(is_hub))
    def _():
        wait_bytes(rows_out, send_sem.at[6])

    @pl.when(is_hub)
    def _():
        wait_bytes(send4.at[pl.ds(0, heads - 1)], send_sem.at[3])

    if spread > 1:

        @pl.when(is_hub & jnp.logical_not(owner))
        def _():
            wait_bytes(send4.at[0], send_sem.at[3])

    def owner_sends():
        for group in range(groups):
            wait_bytes(recv1.at[group, pl.ds(0, n - 1)], send_sem.at[1])
            wait_bytes(recv4.at[pl.ds(0, n - 1)], send_sem.at[4])
        for group in range(groups - 1):
            wait_bytes(recv1.at[group, 0], send_sem.at[1])
            wait_bytes(recv4.at[0], send_sem.at[4])

    when_owner(owner_sends)


def body(
    n,
    cores,
    hidden_state,
    query_weight,
    up_key,
    up_value,
    latent_key,
    latent_value,
    lengths,
    block_mask,
    out_weight,
):
    batch, context_len, _, rank = latent_key.shape
    width = query_weight.shape[2]
    heads = KPG * REP
    model = out_weight.shape[2]
    chunks = model // HD
    f32, bf16 = jnp.float32, jnp.bfloat16
    vmem = pltpu.VMEM
    return pl.pallas_call(
        functools.partial(kernel, n, cores),
        out_shape=pltpu.VMEM((batch, model), f32),
        in_specs=[pl.BlockSpec(memory_space=pl.ANY)] * 9,
        out_specs=pl.BlockSpec(memory_space=pltpu.VMEM),
        scratch_shapes=[
            pltpu.SMEM(lengths.shape, jnp.int32),
            pltpu.SMEM(block_mask.shape[::-1], jnp.int32),
            vmem(hidden_state.shape, bf16),
            vmem((max(query_weight.shape[0], HD), width), bf16),
            vmem(up_key.shape[1:], bf16),
            vmem(up_value.shape[1:], bf16),
            vmem((batch, context_len, rank), bf16),
            vmem((batch, context_len, rank), bf16),
            vmem((max(out_weight.shape[1], HD), model), bf16),
            vmem((heads, batch, HD), f32),
            vmem((cores, n, batch, HD), f32),
            vmem((cores, batch, HD), f32),
            vmem((heads, batch, HD), f32),
            vmem((rank // HD, heads * batch, HD), f32),
            vmem((rank // HD, heads * batch, HD), f32),
            vmem((heads * batch, HD), f32),
            vmem((heads, batch, HD), f32),
            vmem((cores, n, batch, HD), f32),
            vmem((heads, chunks // heads, batch, HD), f32),
            vmem((n, chunks // heads, batch, HD), f32),
            vmem((chunks // heads, batch, HD), f32),
            vmem((heads, chunks // heads, batch, HD), f32),
            vmem((heads, batch, HD), f32),
            vmem((cores, n, batch, HD), f32),
            vmem((max(out_weight.shape[1], HD), model), f32),
            vmem((max(out_weight.shape[1], HD), model), f32),
            vmem((batch, 2 * heads, context_len), bf16),
            pltpu.SemaphoreType.DMA((7,)),
            pltpu.SemaphoreType.DMA((batch,)),
            pltpu.SemaphoreType.DMA((batch,)),
            pltpu.SemaphoreType.DMA((7,)),
            pltpu.SemaphoreType.DMA((7,)),
        ],
        compiler_params=pltpu.CompilerParams(collective_id=0, has_side_effects=True),
    )(
        lengths,
        block_mask.T,
        hidden_state,
        query_weight.reshape(query_weight.shape[0], width),
        up_key.reshape(up_key.shape[1:]),
        up_value.reshape(up_value.shape[1:]),
        latent_key.reshape(batch, context_len, rank),
        latent_value.reshape(batch, context_len, rank),
        out_weight.reshape(out_weight.shape[1:]),
    )


def solution(mesh):
    in_specs = (
        P(),
        P("seq", "head", None),
        P("head", None, None),
        P("head", None, None),
        P(None, "seq", "head", None),
        P(None, "seq", "head", None),
        P(),
        P(None, "seq"),
        P("head", "seq", None),
    )
    return jax.shard_map(
        functools.partial(body, mesh.shape["seq"], mesh.shape["head"]),
        mesh=mesh,
        in_specs=in_specs,
        out_specs=P(),
        check_vma=False,
    )
```

```python
import functools
import math

import jax
import jax.numpy as jnp
from jax import lax
from jax.experimental import pallas as pl
from jax.experimental.pallas import tpu as pltpu
from jax.sharding import PartitionSpec as P

HD = 128
BLOCK = 256
KPG = 4
REP = 4
MESH = pl.DeviceIdType.MESH
NEG = -1e30


def each_other(me, count, step):
    if count <= 32 and count & (count - 1) == 0:
        flips = [(1 << b) * (1 - 2 * lax.rem(me // (1 << b), 2)) for b in range(count.bit_length() - 1)]
        for mask in reversed(range(1, count)):
            step(me + sum(flip for b, flip in enumerate(flips) if mask >> b & 1))
    else:
        lax.fori_loop(0, count - 1, lambda i, c: (step(lax.rem(me + i + 1, count)), c)[1], 0)


def halves(x):
    high = x.astype(jnp.bfloat16)
    low = (x - high.astype(jnp.float32)).astype(jnp.bfloat16)
    return jnp.concatenate([high, low], axis=0)


def dot_nt(a, b):
    return lax.dot_general(a, b, (((1,), (1,)), ((), ())), preferred_element_type=jnp.float32)


def strided(ref, first, count, stride):
    parts = [ref[k, pl.ds(first, count, stride=stride), :] for k in range(ref.shape[0])]
    return jnp.concatenate(parts, axis=1)


def folded(x):
    rows = x.shape[0] // 2
    return x[:rows] + x[rows:]


def kernel(
    n,
    cores,
    lengths_in,
    mask_in,
    hidden_in,
    query_weight,
    up_key,
    up_value,
    keys,
    values,
    out_weight,
    out,
    lengths,
    block_mask,
    hidden,
    qw,
    uk,
    uv,
    kv,
    vv,
    ow,
    send1,
    recv1,
    send2,
    recv2,
    ql,
    ls,
    st,
    send3,
    recv3,
    send4,
    recv4,
    send5,
    recv5,
    send6,
    recv6,
    rows_out,
    rows_in,
    pw,
    load_sem,
    key_sem,
    value_sem,
    send_sem,
    recv_sem,
):
    me = lax.axis_index("seq")
    core = lax.axis_index("head")
    batch, context_len = keys.shape[0], keys.shape[1]
    heads = KPG * REP
    spread = n // heads
    per_owner = send5.shape[0]
    hub = cores - 1
    groups = recv1.shape[0]
    dim_rows, out_rows = query_weight.shape[0], out_weight.shape[0]
    owners, per = send1.shape[0], send1.shape[1]
    first, stride = n // 4, n // 2 // owners
    my_owner = lax.rem(me + n - first, n) // stride
    owner = (me >= first) & (me < first + n // 2) & (lax.rem(me + n - first, stride) == 0)
    is_hub = core == hub

    def local(src, dst, sem):
        return pltpu.make_async_copy(src, dst, sem)

    def remote(src, dst, phase, seq, head):
        return pltpu.make_async_remote_copy(
            src_ref=src,
            dst_ref=dst,
            send_sem=send_sem.at[phase],
            recv_sem=recv_sem.at[phase],
            device_id=(seq, head),
            device_id_type=MESH,
        )

    def wait_bytes(ref, sem):
        local(ref, ref, sem).wait()

    def when_owner(action):
        pl.when(is_hub & owner)(action)

    def each_owner(step):
        base = me * owners // n
        flips = [(1 << b) * (1 - 2 * lax.rem(base // (1 << b), 2)) for b in range(owners.bit_length() - 1)]
        for mask in reversed(range(owners)):
            index = base + sum(flip for b, flip in enumerate(flips) if mask >> b & 1)
            step(index, first + index * stride)

    def to_hub(other, own, src, dst, phase):
        if own is None:
            remote(src, dst, phase, other, hub).start()
        else:

            @pl.when(own)
            def _():
                local(src, dst, recv_sem.at[phase]).start()

            @pl.when(jnp.logical_not(own))
            def _():
                remote(src, dst, phase, other, hub).start()

    if dim_rows >= HD:
        qw_at = qw
    else:
        qw_at = qw.at[pl.ds(pl.multiple_of(lax.rem(me * dim_rows, HD), dim_rows), dim_rows)]
    qw_copy = local(query_weight, qw_at, load_sem.at[0])
    hidden_copy = local(hidden_in, hidden, load_sem.at[4])
    hidden_copy.start()
    qw_copy.start()

    def output_rows():
        if out_rows >= HD:
            return ow[...]
        start = lax.rem(me * out_rows, HD)
        row = lax.broadcasted_iota(jnp.int32, ow.shape, 0)
        kept = jnp.where((row >= start) & (row < start + out_rows), ow[...].astype(jnp.float32), 0.0)
        return kept.astype(jnp.bfloat16)

    barrier = pltpu.get_barrier_semaphore()
    devices = n * cores

    def greet(other):
        pl.semaphore_signal(
            barrier, inc=1, device_id=(other // cores, lax.rem(other, cores)), device_id_type=MESH
        )

    each_other(me * cores + core, devices, greet)

    hidden_copy.wait()
    qw_copy.wait()
    lengths_copy = local(lengths_in, lengths, load_sem.at[5])
    lengths_copy.start()
    mask_copy = local(mask_in, block_mask, load_sem.at[6])
    mask_copy.start()
    uk_copy = local(up_key, uk, load_sem.at[1])
    uk_copy.start()
    key_copies = [local(keys.at[b], kv.at[b], key_sem.at[b]) for b in range(batch)]
    value_copies = [local(values.at[b], vv.at[b], value_sem.at[b]) for b in range(batch)]
    for b in range(batch):
        key_copies[b].start()
        value_copies[b].start()
    uv_copy = local(up_value, uv, load_sem.at[2])
    uv_copy.start()
    if out_rows >= HD:
        ow_at = ow
    else:
        ow_at = ow.at[pl.ds(pl.multiple_of(lax.rem(me * out_rows, HD), out_rows), out_rows)]
    ow_copy = local(out_weight, ow_at, load_sem.at[3])
    ow_copy.start()

    if dim_rows >= HD:
        state = hidden[:, pl.ds(pl.multiple_of(me * dim_rows, HD), dim_rows)]
        weight = qw[...]
    else:
        start = lax.rem(me * dim_rows, HD)
        state = hidden[:, pl.ds(pl.multiple_of(me * dim_rows - start, HD), HD)]
        row = lax.broadcasted_iota(jnp.int32, qw.shape, 0)
        weight = jnp.where((row >= start) & (row < start + dim_rows), qw[...].astype(jnp.float32), 0.0)
        weight = weight.astype(jnp.bfloat16)
    part = jnp.dot(state, weight, preferred_element_type=jnp.float32)
    for h in range(heads):
        send1[h // per, h % per] = part[:, h * HD : (h + 1) * HD]

    pl.semaphore_wait(barrier, devices - 1)

    def send_query(index, chip):
        to_hub(chip, is_hub & (chip == me), send1.at[index], recv1.at[core, me], 0)

    each_owner(send_query)

    ow_copy.wait()

    @pl.when(jnp.logical_not(is_hub))
    def _():
        rows_out[...] = output_rows().astype(jnp.float32)
        remote(rows_out, rows_in, 6, me, hub).start()

    def gather_query():
        wait_bytes(recv1, recv_sem.at[0])
        send2[...] = jnp.sum(recv1[...], axis=1)

        def send(other):
            for group in range(groups):
                remote(send2.at[group], recv2.at[my_owner], 1, other, group).start()

        each_other(me, n, send)
        for group in range(groups - 1):
            remote(send2.at[group], recv2.at[my_owner], 1, me, group).start()
        local(send2.at[hub], recv2.at[my_owner], recv_sem.at[1]).start()

    when_owner(gather_query)
    uk_copy.wait()
    wait_bytes(recv2, recv_sem.at[1])

    scale = 1.0 / math.sqrt(HD)
    rank = uk.shape[0]
    for j in range(KPG):
        rows = jnp.concatenate([recv2[h // per, h % per] for h in range(j * REP, (j + 1) * REP)], axis=0)
        mapped = folded(dot_nt(halves(rows), uk[:, j * HD : (j + 1) * HD])) * scale
        for k in range(rank // HD):
            ql[k, j * REP * batch : (j + 1) * REP * batch, :] = mapped[:, k * HD : (k + 1) * HD]

    lengths_copy.wait()
    mask_copy.wait()
    blocks = context_len // BLOCK
    lane = lax.broadcasted_iota(jnp.int32, (1, BLOCK), 1)
    stat_lane = lax.broadcasted_iota(jnp.int32, (heads, HD), 1)
    for b in range(batch):
        key_copies[b].wait()
    for b in range(batch):
        query = halves(strided(ql, b, heads, batch))
        scores = folded(dot_nt(query, kv[b]))
        limits = [
            jnp.where(block_mask[k, b] == 1, lengths[b] - me * context_len - k * BLOCK, 0)
            for k in range(blocks)
        ]
        valid = jnp.concatenate([lane < limit for limit in limits], axis=1)
        scores = jnp.where(valid, scores, NEG)
        peak = jnp.max(scores, axis=1, keepdims=True)
        weights = jnp.where(valid, jnp.exp(scores - peak), 0.0)
        total = jnp.sum(weights, axis=1, keepdims=True)
        pw[b] = halves(weights)
        st[b * heads : (b + 1) * heads, :] = jnp.where(stat_lane < HD // 2, peak, total)
    for h in range(heads):
        send6[h] = st[pl.ds(h, batch, stride=heads), :]

    def send_stats(other):
        to_hub(other, None, send6.at[other // spread], recv6.at[core, me], 5)

    each_other(me, n, send_stats)
    to_hub(me, is_hub, send6.at[me // spread], recv6.at[core, me], 5)

    for b in range(batch):
        value_copies[b].wait()
    for b in range(batch):
        latent = folded(jnp.dot(pw[b], vv[b], preferred_element_type=jnp.float32))
        for k in range(rank // HD):
            ls[k, b * heads : (b + 1) * heads, :] = latent[:, k * HD : (k + 1) * HD]

    uv_copy.wait()
    for j in range(KPG):
        rows = jnp.concatenate(
            [strided(ls, j * REP + r, batch, heads) for r in range(REP)], axis=0
        )
        summed = folded(
            jnp.dot(halves(rows), uv[:, j * HD : (j + 1) * HD], preferred_element_type=jnp.float32)
        )
        for r in range(REP):
            h = j * REP + r
            send3[h] = summed[r * batch : (r + 1) * batch]

    def send_carry(other):
        to_hub(other, None, send3.at[other // spread], recv3.at[core, me], 2)

    each_other(me, n, send_carry)
    to_hub(me, is_hub, send3.at[me // spread], recv3.at[core, me], 2)

    @pl.when(is_hub)
    def _():
        wait_bytes(rows_in, recv_sem.at[6])
        wait_bytes(recv6, recv_sem.at[5])
        stats = recv6[...]
        turned = pltpu.roll(stats, HD // 2, 3)
        low_lanes = lax.broadcasted_iota(jnp.int32, stats.shape, 3) < HD // 2
        peaks = jnp.where(low_lanes, stats, turned)
        totals = jnp.where(low_lanes, turned, stats)
        factor = jnp.exp(peaks - jnp.max(peaks, axis=1, keepdims=True))
        factor = factor / jnp.sum(totals * factor, axis=1, keepdims=True)
        rows = jnp.concatenate([rows_in[...].astype(jnp.bfloat16), output_rows()], axis=0)

        wait_bytes(recv3, recv_sem.at[2])
        context = jnp.sum(recv3[...] * factor, axis=1).astype(jnp.bfloat16)
        context = jnp.concatenate([context[group] for group in range(groups)], axis=1)
        part = jnp.dot(context, rows, preferred_element_type=jnp.float32)
        for c in range(owners * per_owner):
            send4[c // per_owner, c % per_owner] = part[:, c * HD : (c + 1) * HD]

        def send_part(index, chip):
            to_hub(chip, chip == me, send4.at[index], recv4.at[me], 3)

        each_owner(send_part)

    def gather_out():
        wait_bytes(recv4, recv_sem.at[3])
        send5[...] = jnp.sum(recv4[...], axis=0)

        def send(other):
            for group in range(groups):
                remote(send5, recv5.at[my_owner], 4, other, group).start()

        each_other(me, n, send)
        for group in range(groups - 1):
            remote(send5, recv5.at[my_owner], 4, me, group).start()
        local(send5, recv5.at[my_owner], recv_sem.at[4]).start()

    when_owner(gather_out)
    wait_bytes(recv5, recv_sem.at[4])
    for c in range(owners * per_owner):
        out[:, c * HD : (c + 1) * HD] = recv5[c // per_owner, c % per_owner]

    for phase, piece in ((2, recv3), (5, recv6)):
        wait_bytes(piece.at[0, pl.ds(0, n - 1)], send_sem.at[phase])

        @pl.when(jnp.logical_not(is_hub))
        def _():
            wait_bytes(piece.at[0, 0], send_sem.at[phase])

    wait_bytes(send1.at[pl.ds(0, owners - 1)], send_sem.at[0])

    @pl.when(jnp.logical_not(is_hub & owner))
    def _():
        wait_bytes(send1.at[0], send_sem.at[0])

    @pl.when(jnp.logical_not(is_hub))
    def _():
        wait_bytes(rows_out, send_sem.at[6])

    @pl.when(is_hub)
    def _():
        wait_bytes(send4.at[pl.ds(0, owners - 1)], send_sem.at[3])

    @pl.when(is_hub & jnp.logical_not(owner))
    def _():
        wait_bytes(send4.at[0], send_sem.at[3])

    def owner_sends():
        for group in range(groups):
            wait_bytes(recv1.at[group, pl.ds(0, n - 1)], send_sem.at[1])
            wait_bytes(recv4.at[pl.ds(0, n - 1)], send_sem.at[4])
        for group in range(groups - 1):
            wait_bytes(recv1.at[group, 0], send_sem.at[1])
            wait_bytes(recv4.at[0], send_sem.at[4])

    when_owner(owner_sends)


def body(
    n,
    cores,
    hidden_state,
    query_weight,
    up_key,
    up_value,
    latent_key,
    latent_value,
    lengths,
    block_mask,
    out_weight,
):
    batch, context_len, _, rank = latent_key.shape
    width = query_weight.shape[2]
    heads = KPG * REP
    model = out_weight.shape[2]
    chunks = model // HD
    owners = min(heads, n // 2)
    per = heads // owners
    f32, bf16 = jnp.float32, jnp.bfloat16
    vmem = pltpu.VMEM
    return pl.pallas_call(
        functools.partial(kernel, n, cores),
        out_shape=pltpu.VMEM((batch, model), f32),
        in_specs=[pl.BlockSpec(memory_space=pl.ANY)] * 9,
        out_specs=pl.BlockSpec(memory_space=pltpu.VMEM),
        scratch_shapes=[
            pltpu.SMEM(lengths.shape, jnp.int32),
            pltpu.SMEM(block_mask.shape[::-1], jnp.int32),
            vmem(hidden_state.shape, bf16),
            vmem((max(query_weight.shape[0], HD), width), bf16),
            vmem(up_key.shape[1:], bf16),
            vmem(up_value.shape[1:], bf16),
            vmem((batch, context_len, rank), bf16),
            vmem((batch, context_len, rank), bf16),
            vmem((max(out_weight.shape[1], HD), model), bf16),
            vmem((owners, per, batch, HD), f32),
            vmem((cores, n, per, batch, HD), f32),
            vmem((cores, per, batch, HD), f32),
            vmem((owners, per, batch, HD), f32),
            vmem((rank // HD, heads * batch, HD), f32),
            vmem((rank // HD, heads * batch, HD), f32),
            vmem((heads * batch, HD), f32),
            vmem((heads, batch, HD), f32),
            vmem((cores, n, batch, HD), f32),
            vmem((owners, chunks // owners, batch, HD), f32),
            vmem((n, chunks // owners, batch, HD), f32),
            vmem((chunks // owners, batch, HD), f32),
            vmem((owners, chunks // owners, batch, HD), f32),
            vmem((heads, batch, HD), f32),
            vmem((cores, n, batch, HD), f32),
            vmem((max(out_weight.shape[1], HD), model), f32),
            vmem((max(out_weight.shape[1], HD), model), f32),
            vmem((batch, 2 * heads, context_len), bf16),
            pltpu.SemaphoreType.DMA((7,)),
            pltpu.SemaphoreType.DMA((batch,)),
            pltpu.SemaphoreType.DMA((batch,)),
            pltpu.SemaphoreType.DMA((7,)),
            pltpu.SemaphoreType.DMA((7,)),
        ],
        compiler_params=pltpu.CompilerParams(collective_id=0, has_side_effects=True),
    )(
        lengths,
        block_mask.T,
        hidden_state,
        query_weight.reshape(query_weight.shape[0], width),
        up_key.reshape(up_key.shape[1:]),
        up_value.reshape(up_value.shape[1:]),
        latent_key.reshape(batch, context_len, rank),
        latent_value.reshape(batch, context_len, rank),
        out_weight.reshape(out_weight.shape[1:]),
    )


def solution(mesh):
    in_specs = (
        P(),
        P("seq", "head", None),
        P("head", None, None),
        P("head", None, None),
        P(None, "seq", "head", None),
        P(None, "seq", "head", None),
        P(),
        P(None, "seq"),
        P("head", "seq", None),
    )
    return jax.shard_map(
        functools.partial(body, mesh.shape["seq"], mesh.shape["head"]),
        mesh=mesh,
        in_specs=in_specs,
        out_specs=P(),
        check_vma=False,
    )
```

```python
import functools
import math

import jax
import jax.numpy as jnp
from jax import lax
from jax.experimental import pallas as pl
from jax.experimental.pallas import tpu as pltpu
from jax.sharding import PartitionSpec as P

HD = 128
BLOCK = 256
KPG = 4
REP = 4
MESH = pl.DeviceIdType.MESH
NEG = -1e30


def each_other(me, count, step):
    if count <= 32 and count & (count - 1) == 0:
        flips = [(1 << b) * (1 - 2 * lax.rem(me // (1 << b), 2)) for b in range(count.bit_length() - 1)]
        for mask in reversed(range(1, count)):
            step(me + sum(flip for b, flip in enumerate(flips) if mask >> b & 1))
    else:
        lax.fori_loop(0, count - 1, lambda i, c: (step(lax.rem(me + i + 1, count)), c)[1], 0)


def halves(x):
    high = x.astype(jnp.bfloat16)
    low = (x - high.astype(jnp.float32)).astype(jnp.bfloat16)
    return jnp.concatenate([high, low], axis=0)


def dot_nt(a, b):
    return lax.dot_general(a, b, (((1,), (1,)), ((), ())), preferred_element_type=jnp.float32)


def strided(ref, first, count, stride):
    parts = [ref[k, pl.ds(first, count, stride=stride), :] for k in range(ref.shape[0])]
    return jnp.concatenate(parts, axis=1)


def folded(x):
    rows = x.shape[0] // 2
    return x[:rows] + x[rows:]


def kernel(
    n,
    cores,
    lengths_in,
    mask_in,
    hidden_in,
    query_weight,
    up_key,
    up_value,
    keys,
    values,
    out_weight,
    out,
    lengths,
    block_mask,
    hidden,
    qw,
    uk,
    uv,
    kv,
    vv,
    ow,
    send1,
    recv1,
    send2,
    recv2,
    ql,
    ls,
    st,
    send3,
    recv3,
    send4,
    recv4,
    send5,
    recv5,
    send6,
    recv6,
    rows_out,
    rows_in,
    pw,
    load_sem,
    key_sem,
    value_sem,
    send_sem,
    recv_sem,
):
    me = lax.axis_index("seq")
    core = lax.axis_index("head")
    batch, context_len = keys.shape[0], keys.shape[1]
    heads = KPG * REP
    spread = n // heads
    per_owner = send5.shape[0]
    hub = cores - 1
    groups = recv1.shape[0]
    dim_rows, out_rows = query_weight.shape[0], out_weight.shape[0]
    owners, per = send1.shape[0], send1.shape[1]
    first, stride = n // 4, n // 2 // owners
    my_owner = lax.rem(me + n - first, n) // stride
    owner = (me >= first) & (me < first + n // 2) & (lax.rem(me + n - first, stride) == 0)
    is_hub = core == hub

    def local(src, dst, sem):
        return pltpu.make_async_copy(src, dst, sem)

    def remote(src, dst, phase, seq, head):
        return pltpu.make_async_remote_copy(
            src_ref=src,
            dst_ref=dst,
            send_sem=send_sem.at[phase],
            recv_sem=recv_sem.at[phase],
            device_id=(seq, head),
            device_id_type=MESH,
        )

    def wait_bytes(ref, sem):
        local(ref, ref, sem).wait()

    def when_owner(action):
        pl.when(is_hub & owner)(action)

    def each_owner(step):
        base = me * owners // n
        flips = [(1 << b) * (1 - 2 * lax.rem(base // (1 << b), 2)) for b in range(owners.bit_length() - 1)]
        for mask in reversed(range(owners)):
            index = base + sum(flip for b, flip in enumerate(flips) if mask >> b & 1)
            step(index, first + index * stride)

    def to_hub(other, own, src, dst, phase):
        if own is None:
            remote(src, dst, phase, other, hub).start()
        else:

            @pl.when(own)
            def _():
                local(src, dst, recv_sem.at[phase]).start()

            @pl.when(jnp.logical_not(own))
            def _():
                remote(src, dst, phase, other, hub).start()

    if dim_rows >= HD:
        qw_at = qw
    else:
        qw_at = qw.at[pl.ds(pl.multiple_of(lax.rem(me * dim_rows, HD), dim_rows), dim_rows)]
    qw_copy = local(query_weight, qw_at, load_sem.at[0])
    hidden_copy = local(hidden_in, hidden, load_sem.at[4])
    hidden_copy.start()
    qw_copy.start()

    def output_rows():
        if out_rows >= HD:
            return ow[...]
        start = lax.rem(me * out_rows, HD)
        row = lax.broadcasted_iota(jnp.int32, ow.shape, 0)
        kept = jnp.where((row >= start) & (row < start + out_rows), ow[...].astype(jnp.float32), 0.0)
        return kept.astype(jnp.bfloat16)

    barrier = pltpu.get_barrier_semaphore()
    devices = n * cores

    def greet(other):
        pl.semaphore_signal(
            barrier, inc=1, device_id=(other // cores, lax.rem(other, cores)), device_id_type=MESH
        )

    each_other(me * cores + core, devices, greet)

    hidden_copy.wait()
    qw_copy.wait()
    lengths_copy = local(lengths_in, lengths, load_sem.at[5])
    lengths_copy.start()
    mask_copy = local(mask_in, block_mask, load_sem.at[6])
    mask_copy.start()
    uk_copy = local(up_key, uk, load_sem.at[1])
    uk_copy.start()
    key_copies = [local(keys.at[b], kv.at[b], key_sem.at[b]) for b in range(batch)]
    value_copies = [local(values.at[b], vv.at[b], value_sem.at[b]) for b in range(batch)]
    for b in range(batch):
        key_copies[b].start()
        value_copies[b].start()
    uv_copy = local(up_value, uv, load_sem.at[2])
    uv_copy.start()
    if out_rows >= HD:
        ow_at = ow
    else:
        ow_at = ow.at[pl.ds(pl.multiple_of(lax.rem(me * out_rows, HD), out_rows), out_rows)]
    ow_copy = local(out_weight, ow_at, load_sem.at[3])
    ow_copy.start()

    if dim_rows >= HD:
        state = hidden[:, pl.ds(pl.multiple_of(me * dim_rows, HD), dim_rows)]
        weight = qw[...]
    else:
        start = lax.rem(me * dim_rows, HD)
        state = hidden[:, pl.ds(pl.multiple_of(me * dim_rows - start, HD), HD)]
        row = lax.broadcasted_iota(jnp.int32, qw.shape, 0)
        weight = jnp.where((row >= start) & (row < start + dim_rows), qw[...].astype(jnp.float32), 0.0)
        weight = weight.astype(jnp.bfloat16)
    part = jnp.dot(state, weight, preferred_element_type=jnp.float32)
    for h in range(heads):
        send1[h // per, h % per] = part[:, h * HD : (h + 1) * HD]

    pl.semaphore_wait(barrier, devices - 1)

    def send_query(index, chip):
        to_hub(chip, is_hub & (chip == me), send1.at[index], recv1.at[core, me], 0)

    each_owner(send_query)

    ow_copy.wait()

    @pl.when(jnp.logical_not(is_hub))
    def _():
        rows_out[...] = output_rows().astype(jnp.float32)
        remote(rows_out, rows_in, 6, me, hub).start()

    def gather_query():
        wait_bytes(recv1, recv_sem.at[0])
        send2[...] = jnp.sum(recv1[...], axis=1)

        def send(other):
            for group in range(groups):
                remote(send2.at[group], recv2.at[my_owner], 1, other, group).start()

        each_other(me, n, send)
        for group in range(groups - 1):
            remote(send2.at[group], recv2.at[my_owner], 1, me, group).start()
        local(send2.at[hub], recv2.at[my_owner], recv_sem.at[1]).start()

    when_owner(gather_query)
    uk_copy.wait()
    wait_bytes(recv2, recv_sem.at[1])

    scale = 1.0 / math.sqrt(HD)
    rank = uk.shape[0]
    for j in range(KPG):
        rows = jnp.concatenate([recv2[h // per, h % per] for h in range(j * REP, (j + 1) * REP)], axis=0)
        mapped = folded(dot_nt(halves(rows), uk[:, j * HD : (j + 1) * HD])) * scale
        for k in range(rank // HD):
            ql[k, j * REP * batch : (j + 1) * REP * batch, :] = mapped[:, k * HD : (k + 1) * HD]

    lengths_copy.wait()
    mask_copy.wait()
    blocks = context_len // BLOCK
    lane = lax.broadcasted_iota(jnp.int32, (1, BLOCK), 1)
    stat_lane = lax.broadcasted_iota(jnp.int32, (heads, HD), 1)
    for b in range(batch):
        key_copies[b].wait()
    for b in range(batch):
        query = halves(strided(ql, b, heads, batch))
        scores = folded(dot_nt(query, kv[b]))
        limits = [
            jnp.where(block_mask[k, b] == 1, lengths[b] - me * context_len - k * BLOCK, 0)
            for k in range(blocks)
        ]
        valid = jnp.concatenate([lane < limit for limit in limits], axis=1)
        scores = jnp.where(valid, scores, NEG)
        peak = jnp.max(scores, axis=1, keepdims=True)
        weights = jnp.where(valid, jnp.exp(scores - peak), 0.0)
        total = jnp.sum(weights, axis=1, keepdims=True)
        pw[b] = halves(weights)
        st[b * heads : (b + 1) * heads, :] = jnp.where(stat_lane < HD // 2, peak, total)
    for h in range(heads):
        send6[h] = st[pl.ds(h, batch, stride=heads), :]

    def send_stats(other):
        to_hub(other, None, send6.at[other // spread], recv6.at[core, me], 5)

    each_other(me, n, send_stats)
    to_hub(me, is_hub, send6.at[me // spread], recv6.at[core, me], 5)

    for b in range(batch):
        value_copies[b].wait()
    for b in range(batch):
        latent = folded(jnp.dot(pw[b], vv[b], preferred_element_type=jnp.float32))
        for k in range(rank // HD):
            ls[k, b * heads : (b + 1) * heads, :] = latent[:, k * HD : (k + 1) * HD]

    uv_copy.wait()
    for j in range(KPG):
        rows = jnp.concatenate(
            [strided(ls, j * REP + r, batch, heads) for r in range(REP)], axis=0
        )
        summed = folded(
            jnp.dot(halves(rows), uv[:, j * HD : (j + 1) * HD], preferred_element_type=jnp.float32)
        )
        for r in range(REP):
            h = j * REP + r
            send3[h] = summed[r * batch : (r + 1) * batch]

    def send_carry(other):
        to_hub(other, None, send3.at[other // spread], recv3.at[core, me], 2)

    each_other(me, n, send_carry)
    to_hub(me, is_hub, send3.at[me // spread], recv3.at[core, me], 2)

    @pl.when(is_hub)
    def _():
        wait_bytes(rows_in, recv_sem.at[6])
        wait_bytes(recv6, recv_sem.at[5])
        stats = recv6[...]
        turned = pltpu.roll(stats, HD // 2, 3)
        low_lanes = lax.broadcasted_iota(jnp.int32, stats.shape, 3) < HD // 2
        peaks = jnp.where(low_lanes, stats, turned)
        totals = jnp.where(low_lanes, turned, stats)
        factor = jnp.exp(peaks - jnp.max(peaks, axis=1, keepdims=True))
        factor = factor / jnp.sum(totals * factor, axis=1, keepdims=True)
        rows = jnp.concatenate([rows_in[...].astype(jnp.bfloat16), output_rows()], axis=0)

        wait_bytes(recv3, recv_sem.at[2])
        context = jnp.sum(recv3[...] * factor, axis=1).astype(jnp.bfloat16)
        context = jnp.concatenate([context[group] for group in range(groups)], axis=1)
        part = jnp.dot(context, rows, preferred_element_type=jnp.float32)
        for c in range(owners * per_owner):
            send4[c // per_owner, c % per_owner] = part[:, c * HD : (c + 1) * HD]

        def send_part(index, chip):
            to_hub(chip, chip == me, send4.at[index], recv4.at[me], 3)

        each_owner(send_part)

    def gather_out():
        wait_bytes(recv4, recv_sem.at[3])
        send5[...] = jnp.sum(recv4[...], axis=0)

        def send_to(group):
            def send(other):
                remote(send5, recv5.at[my_owner], 4, other, group).start()

            return send

        for group in range(groups):
            each_other(me, n, send_to(group))
        for group in range(groups - 1):
            remote(send5, recv5.at[my_owner], 4, me, group).start()
        local(send5, recv5.at[my_owner], recv_sem.at[4]).start()

    when_owner(gather_out)
    wait_bytes(recv5, recv_sem.at[4])
    for c in range(owners * per_owner):
        out[:, c * HD : (c + 1) * HD] = recv5[c // per_owner, c % per_owner]

    for phase, piece in ((2, recv3), (5, recv6)):
        wait_bytes(piece.at[0, pl.ds(0, n - 1)], send_sem.at[phase])

        @pl.when(jnp.logical_not(is_hub))
        def _():
            wait_bytes(piece.at[0, 0], send_sem.at[phase])

    wait_bytes(send1.at[pl.ds(0, owners - 1)], send_sem.at[0])

    @pl.when(jnp.logical_not(is_hub & owner))
    def _():
        wait_bytes(send1.at[0], send_sem.at[0])

    @pl.when(jnp.logical_not(is_hub))
    def _():
        wait_bytes(rows_out, send_sem.at[6])

    @pl.when(is_hub)
    def _():
        wait_bytes(send4.at[pl.ds(0, owners - 1)], send_sem.at[3])

    @pl.when(is_hub & jnp.logical_not(owner))
    def _():
        wait_bytes(send4.at[0], send_sem.at[3])

    def owner_sends():
        for group in range(groups):
            wait_bytes(recv1.at[group, pl.ds(0, n - 1)], send_sem.at[1])
            wait_bytes(recv4.at[pl.ds(0, n - 1)], send_sem.at[4])
        for group in range(groups - 1):
            wait_bytes(recv1.at[group, 0], send_sem.at[1])
            wait_bytes(recv4.at[0], send_sem.at[4])

    when_owner(owner_sends)


def body(
    n,
    cores,
    hidden_state,
    query_weight,
    up_key,
    up_value,
    latent_key,
    latent_value,
    lengths,
    block_mask,
    out_weight,
):
    batch, context_len, _, rank = latent_key.shape
    width = query_weight.shape[2]
    heads = KPG * REP
    model = out_weight.shape[2]
    chunks = model // HD
    owners = min(heads, n // 2)
    per = heads // owners
    f32, bf16 = jnp.float32, jnp.bfloat16
    vmem = pltpu.VMEM
    return pl.pallas_call(
        functools.partial(kernel, n, cores),
        out_shape=pltpu.VMEM((batch, model), f32),
        in_specs=[pl.BlockSpec(memory_space=pl.ANY)] * 9,
        out_specs=pl.BlockSpec(memory_space=pltpu.VMEM),
        scratch_shapes=[
            pltpu.SMEM(lengths.shape, jnp.int32),
            pltpu.SMEM(block_mask.shape[::-1], jnp.int32),
            vmem(hidden_state.shape, bf16),
            vmem((max(query_weight.shape[0], HD), width), bf16),
            vmem(up_key.shape[1:], bf16),
            vmem(up_value.shape[1:], bf16),
            vmem((batch, context_len, rank), bf16),
            vmem((batch, context_len, rank), bf16),
            vmem((max(out_weight.shape[1], HD), model), bf16),
            vmem((owners, per, batch, HD), f32),
            vmem((cores, n, per, batch, HD), f32),
            vmem((cores, per, batch, HD), f32),
            vmem((owners, per, batch, HD), f32),
            vmem((rank // HD, heads * batch, HD), f32),
            vmem((rank // HD, heads * batch, HD), f32),
            vmem((heads * batch, HD), f32),
            vmem((heads, batch, HD), f32),
            vmem((cores, n, batch, HD), f32),
            vmem((owners, chunks // owners, batch, HD), f32),
            vmem((n, chunks // owners, batch, HD), f32),
            vmem((chunks // owners, batch, HD), f32),
            vmem((owners, chunks // owners, batch, HD), f32),
            vmem((heads, batch, HD), f32),
            vmem((cores, n, batch, HD), f32),
            vmem((max(out_weight.shape[1], HD), model), f32),
            vmem((max(out_weight.shape[1], HD), model), f32),
            vmem((batch, 2 * heads, context_len), bf16),
            pltpu.SemaphoreType.DMA((7,)),
            pltpu.SemaphoreType.DMA((batch,)),
            pltpu.SemaphoreType.DMA((batch,)),
            pltpu.SemaphoreType.DMA((7,)),
            pltpu.SemaphoreType.DMA((7,)),
        ],
        compiler_params=pltpu.CompilerParams(collective_id=0, has_side_effects=True),
    )(
        lengths,
        block_mask.T,
        hidden_state,
        query_weight.reshape(query_weight.shape[0], width),
        up_key.reshape(up_key.shape[1:]),
        up_value.reshape(up_value.shape[1:]),
        latent_key.reshape(batch, context_len, rank),
        latent_value.reshape(batch, context_len, rank),
        out_weight.reshape(out_weight.shape[1:]),
    )


def solution(mesh):
    in_specs = (
        P(),
        P("seq", "head", None),
        P("head", None, None),
        P("head", None, None),
        P(None, "seq", "head", None),
        P(None, "seq", "head", None),
        P(),
        P(None, "seq"),
        P("head", "seq", None),
    )
    return jax.shard_map(
        functools.partial(body, mesh.shape["seq"], mesh.shape["head"]),
        mesh=mesh,
        in_specs=in_specs,
        out_specs=P(),
        check_vma=False,
    )
```
